32 devices in a mesh: fsdp: 8 (over z, x), dp: 4 (over y, core).
Axes of the slice: x: 2, y: 2, z: 4, core: 2. Of those that a mesh axis runs over, the one named last changes fastest.
Arguments:
- layer_in: bfloat16 [20480, 768], P(('fsdp', 'dp')), may hold values from -6 to 6
- ln1_gain: bfloat16 [768], P('fsdp'), may hold values from 0.5 to 1.5
- ln1_bias: bfloat16 [768], P('fsdp'), may hold values from -1.5 to 1.5
- qkv_weight: bfloat16 [768, 2304], P('fsdp'), may hold values from -0.21875 to 0.21875
- qkv_bias: bfloat16 [2304], P('fsdp'), may hold values from -1.5 to 1.5
- rope_freqs: bfloat16 [768], P('fsdp'), may hold values from -3 to 3
- out_weight: bfloat16 [768, 768], P('fsdp'), may hold values from -1.75 to 1.75
- out_bias: bfloat16 [768], P('fsdp'), may hold values from -1.5 to 1.5
- ln2_gain: bfloat16 [768], P('fsdp'), may hold values from 0.5 to 1.5
- ln2_bias: bfloat16 [768], P('fsdp'), may hold values from -1.5 to 1.5
- fc1_weight: bfloat16 [768, 3072], P('fsdp'), may hold values from -0.21875 to 0.21875
- fc1_bias: bfloat16 [3072], P('fsdp'), may hold values from -1.5 to 1.5
- fc2_weight: bfloat16 [3072, 768], P('fsdp'), may hold values from -0.109375 to 0.109375
- fc2_bias: bfloat16 [768], P('fsdp'), may hold values from -1.5 to 1.5
- image_of: int32 [20480], P(('fsdp', 'dp')), may hold values from 0 to 127, as said below
- patch_row: int32 [20480], P(('fsdp', 'dp')), may hold values from 0 to 23, as said below
- patch_col: int32 [20480], P(('fsdp', 'dp')), may hold values from 0 to 23
- grad_out: bfloat16 [20480, 768], P(('fsdp', 'dp')), may hold values from -6 to 6
Outputs:
- output: bfloat16 [20480, 768], P(('fsdp', 'dp'))
- grad_x: bfloat16 [20480, 768], P(('fsdp', 'dp'))
- grad_ln1_gain: float32 [768], P('fsdp')
- grad_ln1_bias: float32 [768], P('fsdp')
- grad_qkv_weight: float32 [768, 2304], P('fsdp')
- grad_qkv_bias: float32 [2304], P('fsdp')
- grad_rope_freqs: float32 [768], P('fsdp')
- grad_out_weight: float32 [768, 768], P('fsdp')
- grad_out_bias: float32 [768], P('fsdp')
- grad_ln2_gain: float32 [768], P('fsdp')
- grad_ln2_bias: float32 [768], P('fsdp')
- grad_fc1_weight: float32 [768, 3072], P('fsdp')
- grad_fc1_bias: float32 [3072], P('fsdp')
- grad_fc2_weight: float32 [3072, 768], P('fsdp')
- grad_fc2_bias: float32 [768], P('fsdp')
The draws below stay inside these ranges and needn't reach their ends.
Inputs may be any that keep to these rules, and one draw needn't show every extreme that they name: `image_of`: rows with equal values form one image of 14 x 14, 20 x 20 or 24 x 24 patches, or the filler at the end of one device's rows; they stand in consecutive rows of one device. `patch_row`: an image's patches run row by row through its grid.
All inputs are finite; a program needn't handle non-finite values.
Results may differ from the reference program's by a relative error of at most 0.012.
Values may be sent and summed in bfloat16 or wider, within the bound.
A program may use at most 192 MiB of HBM per device.

```python
import jax
import jax.numpy as jnp
from jax import lax

D = 768
H = 12
HD = 64
MLP = 3072
TOK_DEV = 640
SIDE_S = 14
SIDE_M = 20
SIDE_L = 24
IMG_SLOTS = 4
TOKENS = 20480


def layout(key):
    key = jax.random.fold_in(key, 7)
    device_count = TOKENS // TOK_DEV
    kinds = jax.random.randint(key, (device_count, IMG_SLOTS), 0, 3)
    kinds = kinds.at[0, 0].set(2)
    kinds = kinds.at[device_count - 1].set(1)
    side_table = jnp.array([SIDE_S, SIDE_M, SIDE_L], jnp.int32)
    sides = side_table[kinds]
    ends = jnp.cumsum(sides * sides, axis=1)
    places = jnp.arange(TOK_DEV, dtype=jnp.int32)
    slot = jnp.sum((ends[:, None, :] <= places[None, :, None]).astype(jnp.int32), axis=2)
    slot = jnp.minimum(slot, IMG_SLOTS - 1)
    slot_end = jnp.take_along_axis(ends, slot, axis=1)
    slot_side = jnp.take_along_axis(sides, slot, axis=1)
    start = slot_end - slot_side * slot_side
    fits = slot_end <= TOK_DEV
    local = places[None, :] - start
    device_ids = jnp.arange(device_count, dtype=jnp.int32)[:, None]
    image = jnp.where(fits, device_ids * IMG_SLOTS + slot, device_ids * IMG_SLOTS + IMG_SLOTS - 1)
    row_idx = jnp.where(fits, local // slot_side, places[None, :] % SIDE_S)
    col_idx = jnp.where(fits, local % slot_side, places[None, :] // SIDE_S % SIDE_S)
    return (image.reshape(-1), row_idx.reshape(-1), col_idx.reshape(-1))


def draw_image_of(key, part):
    return layout(key)[0].astype(jnp.int32)


def draw_patch_row(key, part):
    return layout(key)[1].astype(jnp.int32)


def draw_patch_col(key, part):
    return layout(key)[2].astype(jnp.int32)


def level_of(key, extent, shards, least, top_value):
    factor_of = 1.0
    for position, parts in shards:
        draws = jax.random.uniform(jax.random.fold_in(jax.random.fold_in(key, 6), position), (parts,), jnp.float32, least / len(shards), top_value / len(shards))
        factor_of = factor_of * jnp.repeat(jnp.exp(draws), extent[position] // parts).reshape((-1,) + (1,) * (len(extent) - 1 - position))
    return factor_of


def gaussian(key, shape, width, bound, split=(), kind=jnp.bfloat16):
    level = level_of(key, shape, split, -0.22, 0.18) if split else 1.0
    values = jax.random.normal(key, shape, jnp.float32) * width * level
    return jnp.minimum(jnp.maximum(values, -bound), bound).astype(kind)


def setup_inputs(seed: int = 0) -> dict:
    arg_keys = jax.random.split(jax.random.key(seed), 19)
    return {
        "layer_in": gaussian(arg_keys[0], (TOKENS, D), 1.0, 6.0, ((0, 32),)),
        "ln1_gain": jnp.clip(1.0 + 0.1 * jax.random.normal(arg_keys[1], (D,), jnp.float32), 0.5, 1.5).astype(jnp.bfloat16),
        "ln1_bias": gaussian(arg_keys[2], (D,), 0.3, 1.5, ((0, 8),)),
        "qkv_weight": gaussian(arg_keys[3], (D, 3 * D), D ** -0.5, 0.21875, ((0, 8),)),
        "qkv_bias": gaussian(arg_keys[4], (3 * D,), 0.3, 1.5, ((0, 8),)),
        "rope_freqs": gaussian(arg_keys[5], (D,), 0.5, 3.0, ((0, 8),)),
        "out_weight": gaussian(arg_keys[6], (D, D), (D // 64) ** -0.5, 1.75, ((0, 8),)),
        "out_bias": gaussian(arg_keys[7], (D,), 0.3, 1.5, ((0, 8),)),
        "ln2_gain": jnp.clip(1.0 + 0.1 * jax.random.normal(arg_keys[8], (D,), jnp.float32), 0.5, 1.5).astype(jnp.bfloat16),
        "ln2_bias": gaussian(arg_keys[9], (D,), 0.3, 1.5, ((0, 8),)),
        "fc1_weight": gaussian(arg_keys[10], (D, MLP), D ** -0.5, 0.21875, ((0, 8),)),
        "fc1_bias": gaussian(arg_keys[11], (MLP,), 0.3, 1.5, ((0, 8),)),
        "fc2_weight": gaussian(arg_keys[12], (MLP, D), MLP ** -0.5, 0.109375, ((0, 8),)),
        "fc2_bias": gaussian(arg_keys[13], (D,), 0.3, 1.5, ((0, 8),)),
        "image_of": draw_image_of(jax.random.fold_in(arg_keys[18], 71), 0),
        "patch_row": draw_patch_row(jax.random.fold_in(arg_keys[18], 71), 0),
        "patch_col": draw_patch_col(jax.random.fold_in(arg_keys[18], 71), 0),
        "grad_out": gaussian(arg_keys[17], (TOKENS, D), 1.0, 6.0, ((0, 32),)),
    }


EPSILON = 1e-06
MASKED = -1e+30
HIGHEST_PREC = lax.Precision.HIGHEST

@jax.custom_vjp
def low(v):
    return lax.optimization_barrier(v.astype(jnp.bfloat16)).astype(jnp.float32)

@jax.custom_vjp
def low_back(v):
    return v

def low_keep(v):
    return (low(v), None)

def low_pass(kept, grad):
    return (grad,)

def back_keep(v):
    return (v, None)

def back_low(kept, grad):
    return (low(grad),)
low.defvjp(low_keep, low_pass)
low_back.defvjp(back_keep, back_low)

def linear(left, right):
    return jnp.dot(left, right, precision=HIGHEST_PREC, preferred_element_type=jnp.float32)

def normed(values, scales, shifts):
    centre = values - lax.optimization_barrier(jnp.mean(values, axis=-1, keepdims=True))
    spread = lax.optimization_barrier(jnp.mean(centre * centre, axis=-1, keepdims=True))
    return centre * lax.rsqrt(spread + EPSILON) * scales + shifts

def rotate(queries, keys_in, frequency, row_pos, col_pos):
    half_dim = queries.shape[-1] // 2
    head_count = queries.shape[1]
    split_at = head_count * half_dim
    along_col = frequency[:split_at].reshape(head_count, half_dim)
    along_row = frequency[split_at:].reshape(head_count, half_dim)
    angles = col_pos[:, None, None] * along_col[None] + row_pos[:, None, None] * along_row[None]
    cosine = jnp.cos(angles)
    sine_part = jnp.sin(angles)

    def turned(operand):
        first_half = operand[..., :half_dim]
        second_half = operand[..., half_dim:]
        return jnp.concatenate([first_half * cosine - second_half * sine_part, first_half * sine_part + second_half * cosine], axis=-1)
    return (turned(queries), turned(keys_in))

def layer_block(params, inputs, image_ids, row_pos, col_pos):
    gain_one, shift_one, qkv_mat, qkv_shift, frequency, out_mat, out_shift, gain_two, shift_two, fc1_mat, fc1_shift, fc2_mat, fc2_shift = params
    token_count = inputs.shape[0]
    normed_one = low(normed(inputs, gain_one, shift_one))
    projected = low_back(linear(normed_one, qkv_mat) + qkv_shift)
    queries = projected[:, :D].reshape(token_count, H, HD)
    keys_in = projected[:, D:2 * D].reshape(token_count, H, HD)
    values_in = projected[:, 2 * D:].reshape(token_count, H, HD)
    query_rot, key_rot = rotate(queries, keys_in, frequency, row_pos, col_pos)
    query_low = low(query_rot)
    key_low = low(key_rot)
    value_low = low(values_in)
    scores = jnp.einsum('qhd,khd->hqk', query_low, key_low, precision=HIGHEST_PREC) * HD ** (-0.5)
    same_image = image_ids[:, None] == image_ids[None, :]
    scores = low_back(jnp.where(same_image[None], scores, MASKED))
    probs = low(jax.nn.softmax(scores, axis=-1))
    mixed = jnp.einsum('hqk,khd->qhd', probs, value_low, precision=HIGHEST_PREC).reshape(token_count, D)
    mixed = low_back(low(mixed))
    branch = low_back(linear(mixed, out_mat) + out_shift)
    middle = inputs + branch
    normed_two = low(normed(middle, gain_two, shift_two))
    hidden = low_back(linear(normed_two, fc1_mat) + fc1_shift)
    active = low(jax.nn.gelu(hidden))
    return middle + linear(active, fc2_mat) + fc2_shift

def reference(layer_in, ln1_gain, ln1_bias, qkv_weight, qkv_bias, rope_freqs, out_weight, out_bias, ln2_gain, ln2_bias, fc1_weight, fc1_bias, fc2_weight, fc2_bias, image_of, patch_row, patch_col, grad_out):
    params = tuple((member.astype(jnp.float32) for member in (ln1_gain, ln1_bias, qkv_weight, qkv_bias, rope_freqs, out_weight, out_bias, ln2_gain, ln2_bias, fc1_weight, fc1_bias, fc2_weight, fc2_bias)))
    block_count = TOKENS // TOK_DEV
    image_ids = image_of.reshape(block_count, TOK_DEV)
    row_pos = patch_row.astype(jnp.float32).reshape(block_count, TOK_DEV)
    col_pos = patch_col.astype(jnp.float32).reshape(block_count, TOK_DEV)
    blocked_layer = jax.checkpoint(layer_block)

    def forward(param_set, inputs):
        stacked = inputs.reshape(block_count, TOK_DEV, D)

        def advance(state_in, pieces):
            return (state_in, blocked_layer(param_set, pieces[0], pieces[1], pieces[2], pieces[3]))
        unused, outputs = lax.scan(advance, None, (stacked, image_ids, row_pos, col_pos))
        return outputs.reshape(TOKENS, D)
    result, pull_back = jax.vjp(forward, params, layer_in.astype(jnp.float32))
    grad_params, grad_inputs = pull_back(grad_out.astype(jnp.float32))
    return (result.astype(jnp.bfloat16), grad_inputs.astype(jnp.bfloat16), grad_params[0], grad_params[1], grad_params[2], grad_params[3], grad_params[4], grad_params[5], grad_params[6], grad_params[7], grad_params[8], grad_params[9], grad_params[10], grad_params[11], grad_params[12])
```

```python
from functools import partial

import jax
import jax.numpy as jnp
from jax import lax
from jax.experimental import pallas as pl
from jax.experimental.pallas import tpu as pltpu
from jax.sharding import PartitionSpec as P

D = 768
H = 12
HD = 64


EPSILON = 1e-06
MASKED = -1e30


MESH = pl.DeviceIdType.MESH


def position(index, count):
    odd = lax.rem(index, 2)
    half = lax.div(index, 2)
    return (1 - odd) * half + odd * (count - 1 - half)


def member(place, count):
    place = lax.rem(place + 2 * count, count)
    back = lax.div(place, count // 2)
    return (1 - back) * 2 * place + back * (2 * (count - 1 - place) + 1)


class Place:
    def __init__(self, count):
        self.count = count
        self.far = count // 2
        self.fsdp = lax.axis_index("fsdp")
        self.dp = lax.axis_index("dp")
        self.plane = lax.div(self.dp, 2)
        self.core = lax.rem(self.dp, 2)
        self.place = position(self.fsdp, count)
        self.ring = (
            (member(self.place + 1, count), self.dp),
            (member(self.place - 1, count), self.dp),
        )
        self.across = (self.fsdp, (1 - self.plane) * 2 + self.core)
        self.twin = (self.fsdp, self.plane * 2 + 1 - self.core)

    def owner(self, direction, step):
        return member(self.place - step if direction == 0 else self.place + step, self.count)

    def greet(self):
        barrier = pltpu.get_barrier_semaphore()
        partners = (self.ring[0], self.ring[1], self.across, self.twin)
        for device in partners:
            pl.semaphore_signal(barrier, inc=1, device_id=device, device_id_type=MESH)
        pl.semaphore_wait(barrier, len(partners))


class Sems:
    def __init__(self, send, recv):
        self.send, self.recv, self.used = send, recv, 0

    def take(self):
        self.used += 1
        return self.send.at[self.used - 1], self.recv.at[self.used - 1]


def remote(src, dst, sems, device):
    return pltpu.make_async_remote_copy(
        src_ref=src, dst_ref=dst, send_sem=sems[0], recv_sem=sems[1], device_id=device, device_id_type=MESH
    )


def rows_at(start, size, unit=16):
    return pl.ds(pl.multiple_of(start, unit), size)


class Gather:
    def __init__(self, where, sems, shard, full, shared, local_sem):
        self.where, self.shard, self.full, self.shared = where, shard, full, shared
        self.rows, self.columns = shard.shape
        self.ring_rows = self.rows - shared
        self.cut = -(-max(self.ring_rows // 2, shared) // 16) * 16
        self.local = pltpu.make_async_copy(
            shard, full.at[rows_at(where.fsdp * self.rows, self.rows)], local_sem
        )
        far = where.far
        take = sems.take
        self.ring_sems = [[take() for _ in range(far)] for _ in range(2)]
        self.across_sems = [[take() for _ in range(far)] for _ in range(2)]
        self.twin_sems = [[take() for _ in range(far)] for _ in range(2)]
        self.twin_across_sems = [[take() for _ in range(far)] for _ in range(2)]
        self.sent = []

    def columns_of(self, core):
        half = self.columns // 2
        return pl.ds(pl.multiple_of(core * half, 128), half)

    def ring_span(self, direction, step):
        start, size = 0, self.ring_rows
        if step == self.where.far:
            start, size = (0, self.cut) if direction == 0 else (self.cut, self.ring_rows - self.cut)
        return start, size

    def ring_view(self, owner, direction, step, core, ref=None):
        start, size = self.ring_span(direction, step)
        start = start + self.where.plane * self.shared
        if ref is None:
            ref, start = self.full, start + owner * self.rows
        return ref.at[rows_at(start, size), self.columns_of(core)]

    def across_view(self, owner, plane, core):
        start = owner * self.rows + plane * (self.rows - self.shared)
        return self.full.at[rows_at(start, self.shared), self.columns_of(core)]

    def push(self, copy):
        copy.start()
        self.sent.append(copy)

    def start(self):
        where = self.where
        self.local.start()
        for direction in range(2):
            src = self.ring_view(None, direction, 1, where.core, self.shard)
            dst = self.ring_view(where.fsdp, direction, 1, where.core)
            self.push(remote(src, dst, self.ring_sems[direction][0], where.ring[direction]))

    def ring_step(self, step):
        where = self.where
        far = where.far
        for direction in range(2):
            owner = where.owner(direction, step)
            view = self.ring_view(owner, direction, step, where.core)
            remote(view, view, self.ring_sems[direction][step - 1], where.ring[direction]).wait_recv()
            if step < far:
                onward = self.ring_view(owner, direction, step + 1, where.core)
                self.push(remote(onward, onward, self.ring_sems[direction][step], where.ring[direction]))
                shared = self.across_view(owner, where.plane, where.core)
                self.push(remote(shared, shared, self.across_sems[direction][step - 1], where.across))
            self.push(remote(view, view, self.twin_sems[direction][step - 1], where.twin))
        if step == far:
            owner = where.owner(0, step)
            shared = self.across_view(owner, where.plane, where.core)
            self.push(remote(shared, shared, self.across_sems[0][step - 1], where.across))

    def across_step(self, step):
        where = self.where
        for direction in range(2 if step < where.far else 1):
            owner = where.owner(direction, step)
            view = self.across_view(owner, 1 - where.plane, where.core)
            remote(view, view, self.across_sems[direction][step - 1], where.across).wait_recv()
            self.push(remote(view, view, self.twin_across_sems[direction][step - 1], where.twin))

    def finish(self):
        where = self.where
        for step in range(1, where.far + 1):
            for direction in range(2):
                owner = where.owner(direction, step)
                view = self.ring_view(owner, direction, step, 1 - where.core)
                remote(view, view, self.twin_sems[direction][step - 1], where.twin).wait_recv()
                if step < where.far or direction == 0:
                    view = self.across_view(owner, 1 - where.plane, 1 - where.core)
                    remote(view, view, self.twin_across_sems[direction][step - 1], where.twin).wait_recv()

    def drain(self):
        for copy in self.sent:
            copy.wait_send()
        self.local.wait()


def gather_kernel(count, names, *refs):
    number = len(names)
    shards, fulls = refs[:number], refs[number : 2 * number]
    send, recv, local = refs[2 * number :]
    where = Place(count)
    where.greet()
    sems = Sems(send, recv)
    flows = [
        Gather(where, sems, shard, full, shard.shape[0] // 3, local.at[i])
        for i, (shard, full) in enumerate(zip(shards, fulls))
    ]
    for flow in flows:
        flow.start()
    far = where.far
    for step in range(1, far + 2):
        for flow in flows:
            if step <= far:
                flow.ring_step(step)
            if step > 1:
                flow.across_step(step - 1)
    for flow in flows:
        flow.finish()
    for flow in flows:
        flow.drain()


def gather(shards, count):
    total = len(shards) * 8 * (count // 2)
    return pl.pallas_call(
        partial(gather_kernel, count, range(len(shards))),
        out_shape=[
            jax.ShapeDtypeStruct((s.shape[0] * count, s.shape[1]), s.dtype) for s in shards
        ],
        in_specs=[pl.BlockSpec(memory_space=pltpu.VMEM)] * len(shards),
        out_specs=[pl.BlockSpec(memory_space=pl.ANY)] * len(shards),
        scratch_shapes=[
            pltpu.SemaphoreType.DMA((total,)),
            pltpu.SemaphoreType.DMA((total,)),
            pltpu.SemaphoreType.DMA((len(shards),)),
        ],
        compiler_params=pltpu.CompilerParams(collective_id=0, has_side_effects=True),
        name="gather_params",
    )(*shards)


class Reduce:
    def __init__(self, where, sems, grad, out, shared, bufs):
        self.where, self.grad, self.out, self.shared = where, grad, out, shared
        self.pair, self.other, self.passing, self.final = bufs
        self.rows, self.columns = out.shape
        self.half = self.columns // 2
        self.ring_rows = self.rows - shared
        self.cut = -(-max(self.ring_rows // 2, shared) // 16) * 16
        far = where.far
        take = sems.take
        count = where.count
        self.pair_sems = [take() for _ in range(count)]
        self.other_sems = [take() for _ in range(count)]
        self.ring_sems = [[take() for _ in range(far)] for _ in range(2)]
        self.final_sems = take()
        self.out_sems = take()
        self.sent = []
        self.order = [(0, far)] + [(d, j) for j in range(far - 1, 0, -1) for d in range(2)] + [(0, 0)]

    @staticmethod
    def shapes(rows, columns, count, shared):
        half, ring_rows = columns // 2, rows - shared
        return [
            pltpu.VMEM((count * rows, half), jnp.bfloat16),
            pltpu.VMEM((count * shared, half), jnp.bfloat16),
            pltpu.VMEM((2, count // 2, ring_rows, half), jnp.bfloat16),
            pltpu.VMEM((ring_rows, half), jnp.bfloat16),
        ]

    @staticmethod
    def copies(count):
        return 2 * count + 2 * (count // 2) + 2

    def target(self, direction, distance):
        return self.where.owner(1 - direction, distance)

    def columns_of(self, core):
        return pl.ds(pl.multiple_of(core * self.half, 128), self.half)

    def push(self, copy):
        copy.start()
        self.sent.append(copy)

    def pair_copy(self, i):
        where = self.where
        rows = rows_at(self.target(*self.order[i]) * self.rows, self.rows)
        return remote(
            self.grad.at[rows, self.columns_of(1 - where.core)], self.pair.at[rows], self.pair_sems[i], where.twin
        )

    def start(self, i):
        self.push(self.pair_copy(i))

    def add_pair(self, i):
        where = self.where
        self.pair_copy(i).wait_recv()
        owner = self.target(*self.order[i])
        rows = rows_at(owner * self.rows, self.rows)
        self.pair[rows, :] = self.pair[rows, :] + self.grad[rows, self.columns_of(where.core)]
        theirs = owner * self.rows + (1 - where.plane) * self.ring_rows
        self.push(
            remote(
                self.pair.at[rows_at(theirs, self.shared)],
                self.other.at[rows_at(owner * self.shared, self.shared)],
                self.other_sems[i],
                where.across,
            )
        )

    def add_other(self, i):
        where = self.where
        owner = self.target(*self.order[i])
        theirs = self.other.at[rows_at(owner * self.shared, self.shared)]
        remote(theirs, theirs, self.other_sems[i], where.across).wait_recv()
        mine = rows_at(owner * self.rows + where.plane * self.ring_rows, self.shared)
        self.pair[mine, :] = self.pair[mine, :] + theirs[...]

    def span(self, direction, step):
        if step > 1:
            return 0, self.ring_rows
        return (0, self.cut) if direction == 0 else (self.cut, self.ring_rows - self.cut)

    def ring_rows_of(self, owner, start, size):
        return rows_at(owner * self.rows + self.where.plane * self.shared + start, size)

    def ring_send(self, step):
        where = self.where
        for direction in range(2):
            start, size = self.span(direction, step)
            owner = self.target(direction, where.far + 1 - step)
            self.push(
                remote(
                    self.pair.at[self.ring_rows_of(owner, start, size)],
                    self.passing.at[direction, step - 1, pl.ds(start, size)],
                    self.ring_sems[direction][step - 1],
                    where.ring[direction],
                )
            )

    def ring_step(self, step):
        where = self.where
        for direction in range(2):
            start, size = self.span(direction, step)
            came = self.passing.at[direction, step - 1, pl.ds(start, size)]
            remote(came, came, self.ring_sems[direction][step - 1], where.ring[direction]).wait_recv()
            if step < where.far:
                owner = self.target(direction, where.far - step)
                rows = self.ring_rows_of(owner, start, size)
                self.pair[rows, :] = self.pair[rows, :] + came[...]
        if step < where.far:
            self.ring_send(step + 1)
            return
        rows = self.ring_rows_of(where.fsdp, 0, self.ring_rows)
        total = self.pair[rows, :].astype(jnp.float32)
        total = total + self.passing[0, step - 1].astype(jnp.float32)
        total = total + self.passing[1, step - 1].astype(jnp.float32)
        self.pair[rows, :] = total.astype(jnp.bfloat16)
        self.push(remote(self.pair.at[rows], self.final, self.final_sems, where.across))

    def finish(self):
        where = self.where
        remote(self.final, self.final, self.final_sems, where.across).wait_recv()
        columns = self.columns_of(where.core)
        plane, shared, ring_rows = where.plane, self.shared, self.ring_rows
        both = self.rows - 2 * shared
        base = where.fsdp * self.rows + plane * shared
        f32 = jnp.float32
        if both:
            mine = self.pair[rows_at(base + (1 - plane) * shared, both), :].astype(f32)
            theirs = self.final[rows_at(plane * shared, both), :].astype(f32)
            self.out[pl.ds(shared, both), columns] = mine + theirs
        mine = self.pair[rows_at(base + plane * (ring_rows - shared), shared), :]
        self.out[rows_at(plane * ring_rows, shared), columns] = mine.astype(f32)
        theirs = self.final[rows_at((1 - plane) * (ring_rows - shared), shared), :]
        self.out[rows_at((1 - plane) * ring_rows, shared), columns] = theirs.astype(f32)
        self.push(remote(self.out.at[:, columns], self.out.at[:, columns], self.out_sems, where.twin))

    def close(self):
        where = self.where
        view = self.out.at[:, self.columns_of(1 - where.core)]
        remote(view, view, self.out_sems, where.twin).wait_recv()
        for copy in self.sent:
            copy.wait_send()


def reduce_kernel(count, shares, *refs):
    number = len(shares)
    grads, outs = refs[:number], refs[number : 2 * number]
    send, recv = refs[2 * number : 2 * number + 2]
    bufs = refs[2 * number + 2 :]
    where = Place(count)
    where.greet()
    sems = Sems(send, recv)
    flows = [
        Reduce(where, sems, grad, out, shared, bufs[4 * i : 4 * i + 4])
        for i, (grad, out, shared) in enumerate(zip(grads, outs, shares))
    ]
    far = where.far
    for flow in flows:
        for i in range(count):
            flow.start(i)
    for wave in range(number + far + 1):
        for w, flow in enumerate(flows):
            stage = wave - w
            if stage == 0:
                for i in range(count):
                    flow.add_pair(i)
                for i in range(count):
                    flow.add_other(i)
                    if i == 0:
                        flow.ring_send(1)
            elif 1 <= stage <= far:
                flow.ring_step(stage)
            elif stage == far + 1:
                flow.finish()
    for flow in flows:
        flow.close()


def reduce(grads, shares, count):
    copies = len(grads) * Reduce.copies(count)
    shapes = [(g.shape[0] // count, g.shape[1]) for g in grads]
    return pl.pallas_call(
        partial(reduce_kernel, count, shares),
        out_shape=[jax.ShapeDtypeStruct(s, jnp.float32) for s in shapes],
        in_specs=[pl.BlockSpec(memory_space=pltpu.VMEM)] * len(grads),
        out_specs=[pl.BlockSpec(memory_space=pltpu.VMEM)] * len(grads),
        scratch_shapes=[
            pltpu.SemaphoreType.DMA((copies,)),
            pltpu.SemaphoreType.DMA((copies,)),
        ]
        + [b for s, shared in zip(shapes, shares) for b in Reduce.shapes(*s, count, shared)],
        compiler_params=pltpu.CompilerParams(
            collective_id=1, has_side_effects=True, vmem_limit_bytes=60 << 20
        ),
        name="reduce_grads",
    )(*grads)


def normed(values, scales, shifts):
    centre = values - jnp.mean(values, axis=-1, keepdims=True)
    spread = jnp.mean(centre * centre, axis=-1, keepdims=True)
    return centre * lax.rsqrt(spread + EPSILON) * scales + shifts


def rotate(queries, keys_in, frequency, row_pos, col_pos):
    half_dim = queries.shape[-1] // 2
    head_count = queries.shape[1]
    split_at = head_count * half_dim
    along_col = frequency[:split_at].reshape(head_count, half_dim)
    along_row = frequency[split_at:].reshape(head_count, half_dim)
    angles = col_pos[:, None, None] * along_col[None] + row_pos[:, None, None] * along_row[None]
    cosine = jnp.cos(angles)
    sine_part = jnp.sin(angles)

    def turned(operand):
        first_half = operand[..., :half_dim]
        second_half = operand[..., half_dim:]
        return jnp.concatenate(
            [
                first_half * cosine - second_half * sine_part,
                first_half * sine_part + second_half * cosine,
            ],
            axis=-1,
        )

    return (turned(queries), turned(keys_in))


def body(
    layer_in,
    ln1_gain,
    ln1_bias,
    qkv_weight,
    qkv_bias,
    rope_freqs,
    out_weight,
    out_bias,
    ln2_gain,
    ln2_bias,
    fc1_weight,
    fc1_bias,
    fc2_weight,
    fc2_bias,
    image_of,
    patch_row,
    patch_col,
    grad_out,
):
    gathered = (
        lax.all_gather(ln1_gain, "fsdp", axis=0, tiled=True),
        lax.all_gather(ln1_bias, "fsdp", axis=0, tiled=True),
        lax.all_gather(qkv_weight, "fsdp", axis=0, tiled=True),
        lax.all_gather(qkv_bias, "fsdp", axis=0, tiled=True),
        lax.all_gather(rope_freqs, "fsdp", axis=0, tiled=True),
        lax.all_gather(out_weight, "fsdp", axis=0, tiled=True),
        lax.all_gather(out_bias, "fsdp", axis=0, tiled=True),
        lax.all_gather(ln2_gain, "fsdp", axis=0, tiled=True),
        lax.all_gather(ln2_bias, "fsdp", axis=0, tiled=True),
        lax.all_gather(fc1_weight, "fsdp", axis=0, tiled=True),
        lax.all_gather(fc1_bias, "fsdp", axis=0, tiled=True),
        lax.all_gather(fc2_weight, "fsdp", axis=0, tiled=True),
        lax.all_gather(fc2_bias, "fsdp", axis=0, tiled=True),
    )
    (
        gain_one,
        shift_one,
        qkv_mat,
        qkv_shift,
        frequency,
        out_mat,
        out_shift,
        gain_two,
        shift_two,
        fc1_mat,
        fc1_shift,
        fc2_mat,
        fc2_shift,
    ) = gathered
    token_count = layer_in.shape[0]
    inputs = layer_in.astype(jnp.float32)
    row_pos = patch_row.astype(jnp.float32)
    col_pos = patch_col.astype(jnp.float32)
    scale_qk = HD ** (-0.5)
    same_image = image_of[:, None] == image_of[None, :]
    normed_one, norm_one_pull = jax.vjp(
        normed, inputs, gain_one.astype(jnp.float32), shift_one.astype(jnp.float32)
    )
    normed_one_low = normed_one.astype(jnp.bfloat16)
    projected = jnp.dot(
        normed_one_low, qkv_mat, preferred_element_type=jnp.float32
    ) + qkv_shift.astype(jnp.float32)
    queries = projected[:, :D].reshape(token_count, H, HD)
    keys_in = projected[:, D : 2 * D].reshape(token_count, H, HD)
    values_in = projected[:, 2 * D :].reshape(token_count, H, HD)
    rotation = partial(rotate, row_pos=row_pos, col_pos=col_pos)
    (query_rot, key_rot), rope_pull = jax.vjp(
        rotation, queries, keys_in, frequency.astype(jnp.float32)
    )
    query_heads = query_rot.astype(jnp.bfloat16).transpose(1, 0, 2)
    key_heads = key_rot.astype(jnp.bfloat16).transpose(1, 0, 2)
    value_heads = values_in.astype(jnp.bfloat16).transpose(1, 0, 2)

    def head_scores(query_one, key_one):
        scores = (
            jnp.einsum("qd,kd->qk", query_one, key_one, preferred_element_type=jnp.float32)
            * scale_qk
        )
        return jnp.where(same_image, scores, MASKED)

    def head_forward(operands):
        query_one, key_one, value_one = operands
        scores = head_scores(query_one, key_one)
        peak_score = jnp.max(scores, axis=-1, keepdims=True)
        log_total = peak_score + jnp.log(
            jnp.sum(jnp.exp(scores - peak_score), axis=-1, keepdims=True)
        )
        probs = jnp.exp(scores - log_total)
        mixed_one = jnp.dot(
            probs.astype(jnp.bfloat16), value_one, preferred_element_type=jnp.float32
        )
        return (mixed_one, log_total[:, 0])

    mixed_heads, log_totals = lax.map(head_forward, (query_heads, key_heads, value_heads))
    mixed_low = mixed_heads.transpose(1, 0, 2).reshape(token_count, D).astype(jnp.bfloat16)
    middle = (
        inputs
        + jnp.dot(mixed_low, out_mat, preferred_element_type=jnp.float32)
        + out_shift.astype(jnp.float32)
    )
    normed_two, norm_two_pull = jax.vjp(
        normed, middle, gain_two.astype(jnp.float32), shift_two.astype(jnp.float32)
    )
    normed_two_low = normed_two.astype(jnp.bfloat16)
    hidden = jnp.dot(
        normed_two_low, fc1_mat, preferred_element_type=jnp.float32
    ) + fc1_shift.astype(jnp.float32)
    active, gelu_pull = jax.vjp(jax.nn.gelu, hidden)
    active_low = active.astype(jnp.bfloat16)
    result = (
        middle
        + jnp.dot(active_low, fc2_mat, preferred_element_type=jnp.float32)
        + fc2_shift.astype(jnp.float32)
    )
    output = result.astype(jnp.bfloat16)
    again = (
        lax.all_gather(ln1_gain, "fsdp", axis=0, tiled=True),
        lax.all_gather(ln1_bias, "fsdp", axis=0, tiled=True),
        lax.all_gather(qkv_weight, "fsdp", axis=0, tiled=True),
        lax.all_gather(qkv_bias, "fsdp", axis=0, tiled=True),
        lax.all_gather(rope_freqs, "fsdp", axis=0, tiled=True),
        lax.all_gather(out_weight, "fsdp", axis=0, tiled=True),
        lax.all_gather(out_bias, "fsdp", axis=0, tiled=True),
        lax.all_gather(ln2_gain, "fsdp", axis=0, tiled=True),
        lax.all_gather(ln2_bias, "fsdp", axis=0, tiled=True),
        lax.all_gather(fc1_weight, "fsdp", axis=0, tiled=True),
        lax.all_gather(fc1_bias, "fsdp", axis=0, tiled=True),
        lax.all_gather(fc2_weight, "fsdp", axis=0, tiled=True),
        lax.all_gather(fc2_bias, "fsdp", axis=0, tiled=True),
    )
    qkv_back = again[2]
    out_back = again[5]
    fc1_back = again[9]
    fc2_back = again[11]
    upstream = grad_out.astype(jnp.float32)
    grad_fc2 = jnp.einsum("ti,to->io", active_low, grad_out, preferred_element_type=jnp.float32)
    grad_fc2_shift = jnp.sum(upstream, axis=0)
    grad_active = jnp.einsum("to,io->ti", grad_out, fc2_back, preferred_element_type=jnp.float32)
    (grad_hidden,) = gelu_pull(grad_active)
    grad_hidden_low = grad_hidden.astype(jnp.bfloat16)
    grad_fc1 = jnp.einsum(
        "td,th->dh", normed_two_low, grad_hidden_low, preferred_element_type=jnp.float32
    )
    grad_fc1_shift = jnp.sum(grad_hidden_low.astype(jnp.float32), axis=0)
    grad_normed_two = jnp.einsum(
        "th,dh->td", grad_hidden_low, fc1_back, preferred_element_type=jnp.float32
    )
    grad_middle_norm, grad_gain_two, grad_shift_two = norm_two_pull(grad_normed_two)
    grad_middle = upstream + grad_middle_norm
    grad_middle_low = grad_middle.astype(jnp.bfloat16)
    grad_out_shift = jnp.sum(grad_middle_low.astype(jnp.float32), axis=0)
    grad_out_mat = jnp.einsum(
        "ti,to->io", mixed_low, grad_middle_low, preferred_element_type=jnp.float32
    )
    grad_mixed = jnp.einsum(
        "to,io->ti", grad_middle_low, out_back, preferred_element_type=jnp.float32
    )
    grad_mixed_heads = (
        grad_mixed.astype(jnp.bfloat16).reshape(token_count, H, HD).transpose(1, 0, 2)
    )

    def head_backward(operands):
        query_one, key_one, value_one, grad_one, log_total = operands
        scores = head_scores(query_one, key_one)
        probs = jnp.exp(scores - log_total[:, None])
        grad_value = jnp.einsum(
            "qk,qd->kd", probs.astype(jnp.bfloat16), grad_one, preferred_element_type=jnp.float32
        )
        grad_probs = jnp.einsum(
            "qd,kd->qk", grad_one, value_one, preferred_element_type=jnp.float32
        )
        grad_scores = probs * (grad_probs - jnp.sum(probs * grad_probs, axis=-1, keepdims=True))
        grad_scores_low = grad_scores.astype(jnp.bfloat16)
        grad_query = (
            jnp.einsum("qk,kd->qd", grad_scores_low, key_one, preferred_element_type=jnp.float32)
            * scale_qk
        )
        grad_key = (
            jnp.einsum("qk,qd->kd", grad_scores_low, query_one, preferred_element_type=jnp.float32)
            * scale_qk
        )
        return (grad_query, grad_key, grad_value)

    grad_query_heads, grad_key_heads, grad_value_heads = lax.map(
        head_backward, (query_heads, key_heads, value_heads, grad_mixed_heads, log_totals)
    )
    grad_query_rot = grad_query_heads.transpose(1, 0, 2)
    grad_key_rot = grad_key_heads.transpose(1, 0, 2)
    grad_values = grad_value_heads.transpose(1, 0, 2)
    grad_queries, grad_keys, grad_frequency = rope_pull((grad_query_rot, grad_key_rot))
    grad_projected = jnp.concatenate(
        [
            grad_queries.reshape(token_count, D),
            grad_keys.reshape(token_count, D),
            grad_values.reshape(token_count, D),
        ],
        axis=1,
    ).astype(jnp.bfloat16)
    grad_qkv_shift = jnp.sum(grad_projected.astype(jnp.float32), axis=0)
    grad_qkv = jnp.einsum(
        "td,tp->dp", normed_one_low, grad_projected, preferred_element_type=jnp.float32
    )
    grad_normed_one = jnp.einsum(
        "tp,dp->td", grad_projected, qkv_back, preferred_element_type=jnp.float32
    )
    grad_input_norm, grad_gain_one, grad_shift_one = norm_one_pull(grad_normed_one)
    grad_x = (grad_middle + grad_input_norm).astype(jnp.bfloat16)
    owned = (
        lax.psum_scatter(grad_gain_one, "fsdp", scatter_dimension=0, tiled=True),
        lax.psum_scatter(grad_shift_one, "fsdp", scatter_dimension=0, tiled=True),
        lax.psum_scatter(grad_qkv, "fsdp", scatter_dimension=0, tiled=True),
        lax.psum_scatter(grad_qkv_shift, "fsdp", scatter_dimension=0, tiled=True),
        lax.psum_scatter(grad_frequency, "fsdp", scatter_dimension=0, tiled=True),
        lax.psum_scatter(grad_out_mat, "fsdp", scatter_dimension=0, tiled=True),
        lax.psum_scatter(grad_out_shift, "fsdp", scatter_dimension=0, tiled=True),
        lax.psum_scatter(grad_gain_two, "fsdp", scatter_dimension=0, tiled=True),
        lax.psum_scatter(grad_shift_two, "fsdp", scatter_dimension=0, tiled=True),
        lax.psum_scatter(grad_fc1, "fsdp", scatter_dimension=0, tiled=True),
        lax.psum_scatter(grad_fc1_shift, "fsdp", scatter_dimension=0, tiled=True),
        lax.psum_scatter(grad_fc2, "fsdp", scatter_dimension=0, tiled=True),
        lax.psum_scatter(grad_fc2_shift, "fsdp", scatter_dimension=0, tiled=True),
    )
    summed = lax.psum(
        (
            owned[0],
            owned[1],
            owned[2],
            owned[3],
            owned[4],
            owned[5],
            owned[6],
            owned[7],
            owned[8],
            owned[9],
            owned[10],
            owned[11],
            owned[12],
        ),
        "dp",
    )
    return (
        output,
        grad_x,
        summed[0],
        summed[1],
        summed[2],
        summed[3],
        summed[4],
        summed[5],
        summed[6],
        summed[7],
        summed[8],
        summed[9],
        summed[10],
        summed[11],
        summed[12],
    )


def fast_body(
    layer_in,
    ln1_gain,
    ln1_bias,
    qkv_weight,
    qkv_bias,
    rope_freqs,
    out_weight,
    out_bias,
    ln2_gain,
    ln2_bias,
    fc1_weight,
    fc1_bias,
    fc2_weight,
    fc2_bias,
    image_of,
    patch_row,
    patch_col,
    grad_out,
):
    small = (ln1_gain, ln1_bias, qkv_bias, rope_freqs, out_bias, ln2_gain, ln2_bias, fc1_bias, fc2_bias)
    count = lax.axis_size("fsdp")
    qkv_mat, out_mat, fc1_mat, fc2_mat = gather((qkv_weight, out_weight, fc1_weight, fc2_weight), count)
    packed = lax.all_gather(jnp.concatenate(small), "fsdp", axis=0)
    wholes, start = [], 0
    for vector in small:
        wholes.append(packed[:, start : start + vector.shape[0]].reshape(-1))
        start += vector.shape[0]
    gain_one, shift_one, qkv_shift, frequency, out_shift, gain_two, shift_two, fc1_shift, fc2_shift = wholes
    token_count = layer_in.shape[0]
    inputs = layer_in.astype(jnp.float32)
    row_pos = patch_row.astype(jnp.float32)
    col_pos = patch_col.astype(jnp.float32)
    scale_qk = HD ** (-0.5)
    same_image = image_of[:, None] == image_of[None, :]
    normed_one, norm_one_pull = jax.vjp(
        normed, inputs, gain_one.astype(jnp.float32), shift_one.astype(jnp.float32)
    )
    normed_one_low = normed_one.astype(jnp.bfloat16)
    projected = jnp.dot(
        normed_one_low, qkv_mat, preferred_element_type=jnp.float32
    ) + qkv_shift.astype(jnp.float32)
    queries = projected[:, :D].reshape(token_count, H, HD)
    keys_in = projected[:, D : 2 * D].reshape(token_count, H, HD)
    values_in = projected[:, 2 * D :].reshape(token_count, H, HD)
    rotation = partial(rotate, row_pos=row_pos, col_pos=col_pos)
    (query_rot, key_rot), rope_pull = jax.vjp(
        rotation, queries, keys_in, frequency.astype(jnp.float32)
    )
    query_heads = query_rot.astype(jnp.bfloat16).transpose(1, 0, 2)
    key_heads = key_rot.astype(jnp.bfloat16).transpose(1, 0, 2)
    value_heads = values_in.astype(jnp.bfloat16).transpose(1, 0, 2)

    def head_scores(query_one, key_one):
        scores = (
            jnp.einsum("qd,kd->qk", query_one, key_one, preferred_element_type=jnp.float32)
            * scale_qk
        )
        return jnp.where(same_image, scores, MASKED)

    def head_forward(operands):
        query_one, key_one, value_one = operands
        scores = head_scores(query_one, key_one)
        peak_score = jnp.max(scores, axis=-1, keepdims=True)
        log_total = peak_score + jnp.log(
            jnp.sum(jnp.exp(scores - peak_score), axis=-1, keepdims=True)
        )
        probs = jnp.exp(scores - log_total)
        mixed_one = jnp.dot(
            probs.astype(jnp.bfloat16), value_one, preferred_element_type=jnp.float32
        )
        return (mixed_one, log_total[:, 0])

    mixed_heads, log_totals = lax.map(head_forward, (query_heads, key_heads, value_heads))
    mixed_low = mixed_heads.transpose(1, 0, 2).reshape(token_count, D).astype(jnp.bfloat16)
    middle = (
        inputs
        + jnp.dot(mixed_low, out_mat, preferred_element_type=jnp.float32)
        + out_shift.astype(jnp.float32)
    )
    normed_two, norm_two_pull = jax.vjp(
        normed, middle, gain_two.astype(jnp.float32), shift_two.astype(jnp.float32)
    )
    normed_two_low = normed_two.astype(jnp.bfloat16)
    hidden = jnp.dot(
        normed_two_low, fc1_mat, preferred_element_type=jnp.float32
    ) + fc1_shift.astype(jnp.float32)
    active, gelu_pull = jax.vjp(jax.nn.gelu, hidden)
    active_low = active.astype(jnp.bfloat16)
    result = (
        middle
        + jnp.dot(active_low, fc2_mat, preferred_element_type=jnp.float32)
        + fc2_shift.astype(jnp.float32)
    )
    output = result.astype(jnp.bfloat16)
    qkv_back, out_back, fc1_back, fc2_back = qkv_mat, out_mat, fc1_mat, fc2_mat
    upstream = grad_out.astype(jnp.float32)
    grad_fc2 = jnp.einsum("ti,to->io", active_low, grad_out, preferred_element_type=jnp.float32)
    grad_fc2_shift = jnp.sum(upstream, axis=0)
    grad_active = jnp.einsum("to,io->ti", grad_out, fc2_back, preferred_element_type=jnp.float32)
    (grad_hidden,) = gelu_pull(grad_active)
    grad_hidden_low = grad_hidden.astype(jnp.bfloat16)
    grad_fc1 = jnp.einsum(
        "td,th->dh", normed_two_low, grad_hidden_low, preferred_element_type=jnp.float32
    )
    grad_fc1_shift = jnp.sum(grad_hidden_low.astype(jnp.float32), axis=0)
    grad_normed_two = jnp.einsum(
        "th,dh->td", grad_hidden_low, fc1_back, preferred_element_type=jnp.float32
    )
    grad_middle_norm, grad_gain_two, grad_shift_two = norm_two_pull(grad_normed_two)
    grad_middle = upstream + grad_middle_norm
    grad_middle_low = grad_middle.astype(jnp.bfloat16)
    grad_out_shift = jnp.sum(grad_middle_low.astype(jnp.float32), axis=0)
    grad_out_mat = jnp.einsum(
        "ti,to->io", mixed_low, grad_middle_low, preferred_element_type=jnp.float32
    )
    grad_mixed = jnp.einsum(
        "to,io->ti", grad_middle_low, out_back, preferred_element_type=jnp.float32
    )
    grad_mixed_heads = (
        grad_mixed.astype(jnp.bfloat16).reshape(token_count, H, HD).transpose(1, 0, 2)
    )

    def head_backward(operands):
        query_one, key_one, value_one, grad_one, log_total = operands
        scores = head_scores(query_one, key_one)
        probs = jnp.exp(scores - log_total[:, None])
        grad_value = jnp.einsum(
            "qk,qd->kd", probs.astype(jnp.bfloat16), grad_one, preferred_element_type=jnp.float32
        )
        grad_probs = jnp.einsum(
            "qd,kd->qk", grad_one, value_one, preferred_element_type=jnp.float32
        )
        grad_scores = probs * (grad_probs - jnp.sum(probs * grad_probs, axis=-1, keepdims=True))
        grad_scores_low = grad_scores.astype(jnp.bfloat16)
        grad_query = (
            jnp.einsum("qk,kd->qd", grad_scores_low, key_one, preferred_element_type=jnp.float32)
            * scale_qk
        )
        grad_key = (
            jnp.einsum("qk,qd->kd", grad_scores_low, query_one, preferred_element_type=jnp.float32)
            * scale_qk
        )
        return (grad_query, grad_key, grad_value)

    grad_query_heads, grad_key_heads, grad_value_heads = lax.map(
        head_backward, (query_heads, key_heads, value_heads, grad_mixed_heads, log_totals)
    )
    grad_query_rot = grad_query_heads.transpose(1, 0, 2)
    grad_key_rot = grad_key_heads.transpose(1, 0, 2)
    grad_values = grad_value_heads.transpose(1, 0, 2)
    grad_queries, grad_keys, grad_frequency = rope_pull((grad_query_rot, grad_key_rot))
    grad_projected = jnp.concatenate(
        [
            grad_queries.reshape(token_count, D),
            grad_keys.reshape(token_count, D),
            grad_values.reshape(token_count, D),
        ],
        axis=1,
    ).astype(jnp.bfloat16)
    grad_qkv_shift = jnp.sum(grad_projected.astype(jnp.float32), axis=0)
    grad_qkv = jnp.einsum(
        "td,tp->dp", normed_one_low, grad_projected, preferred_element_type=jnp.float32
    )
    grad_normed_one = jnp.einsum(
        "tp,dp->td", grad_projected, qkv_back, preferred_element_type=jnp.float32
    )
    grad_input_norm, grad_gain_one, grad_shift_one = norm_one_pull(grad_normed_one)
    grad_x = (grad_middle + grad_input_norm).astype(jnp.bfloat16)
    low = tuple(g.astype(jnp.bfloat16) for g in (grad_fc2, grad_fc1, grad_out_mat, grad_qkv))
    shares = tuple(16 * (g.shape[0] // count // 64) for g in low)
    grad_fc2, grad_fc1, grad_out_mat, grad_qkv = reduce(low, shares, count)
    sums = (
        grad_gain_one,
        grad_shift_one,
        grad_qkv_shift,
        grad_frequency,
        grad_out_shift,
        grad_gain_two,
        grad_shift_two,
        grad_fc1_shift,
        grad_fc2_shift,
    )
    whole = lax.psum(jnp.concatenate(sums), ("fsdp", "dp"))
    owned, start = [], 0
    for vector in sums:
        size = vector.shape[0] // count
        owned.append(lax.dynamic_slice(whole, (start + lax.axis_index("fsdp") * size,), (size,)))
        start += vector.shape[0]
    return (
        output,
        grad_x,
        owned[0],
        owned[1],
        grad_qkv,
        owned[2],
        owned[3],
        grad_out_mat,
        owned[4],
        owned[5],
        owned[6],
        grad_fc1,
        owned[7],
        grad_fc2,
        owned[8],
    )


def fits(mesh):
    count = mesh.shape["fsdp"]
    return count % 2 == 0 and count >= 4 and mesh.shape["dp"] == 4 and D % (96 * count) == 0


def solution(mesh):
    in_specs = (
        P(("fsdp", "dp"), None),
        P("fsdp"),
        P("fsdp"),
        P("fsdp", None),
        P("fsdp"),
        P("fsdp"),
        P("fsdp", None),
        P("fsdp"),
        P("fsdp"),
        P("fsdp"),
        P("fsdp", None),
        P("fsdp"),
        P("fsdp", None),
        P("fsdp"),
        P(("fsdp", "dp")),
        P(("fsdp", "dp")),
        P(("fsdp", "dp")),
        P(("fsdp", "dp"), None),
    )
    out_specs = (
        P(("fsdp", "dp"), None),
        P(("fsdp", "dp"), None),
        P("fsdp"),
        P("fsdp"),
        P("fsdp", None),
        P("fsdp"),
        P("fsdp"),
        P("fsdp", None),
        P("fsdp"),
        P("fsdp"),
        P("fsdp"),
        P("fsdp", None),
        P("fsdp"),
        P("fsdp", None),
        P("fsdp"),
    )
    return jax.shard_map(fast_body if fits(mesh) else body, mesh=mesh, in_specs=in_specs, out_specs=out_specs, check_vma=False)
```

```python
import math
from functools import partial

import jax
import jax.numpy as jnp
from jax import lax
from jax.experimental import pallas as pl
from jax.experimental.pallas import tpu as pltpu
from jax.sharding import PartitionSpec as P

D = 768
H = 12
HD = 64
EPSILON = 1e-06
MASKED = -1e30

MESH = pl.DeviceIdType.MESH


def position(index, count):
    odd = lax.rem(index, 2)
    half = lax.div(index, 2)
    return (1 - odd) * half + odd * (count - 1 - half)


def member(place, count):
    place = lax.rem(place + 2 * count, count)
    back = lax.div(place, count // 2)
    return (1 - back) * 2 * place + back * (2 * (count - 1 - place) + 1)


class Place:
    def __init__(self, count):
        self.count = count
        self.far = count // 2
        self.fsdp = lax.axis_index("fsdp")
        self.dp = lax.axis_index("dp")
        self.plane = lax.div(self.dp, 2)
        self.core = lax.rem(self.dp, 2)
        self.place = position(self.fsdp, count)
        self.ring = (
            (member(self.place + 1, count), self.dp),
            (member(self.place - 1, count), self.dp),
        )
        self.across = (self.fsdp, (1 - self.plane) * 2 + self.core)
        self.twin = (self.fsdp, self.plane * 2 + 1 - self.core)

    def owner(self, direction, step):
        return member(self.place - step if direction == 0 else self.place + step, self.count)

    def greet(self, peers=None):
        barrier = pltpu.get_barrier_semaphore()
        partners = tuple(self.ring if peers is None else peers) + (self.across, self.twin)
        for device in partners:
            pl.semaphore_signal(barrier, inc=1, device_id=device, device_id_type=MESH)
        pl.semaphore_wait(barrier, len(partners))


class Sems:
    def __init__(self, send, recv):
        self.send, self.recv, self.used = send, recv, 0

    def take(self):
        self.used += 1
        return self.send.at[self.used - 1], self.recv.at[self.used - 1]


def remote(src, dst, sems, device):
    return pltpu.make_async_remote_copy(
        src_ref=src, dst_ref=dst, send_sem=sems[0], recv_sem=sems[1], device_id=device, device_id_type=MESH
    )


def rows_at(start, size, unit=16):
    return pl.ds(pl.multiple_of(start, unit), size)


class Gather:
    def __init__(self, where, sems, shard, full, shared, local_sem):
        self.where, self.shard, self.full, self.shared = where, shard, full, shared
        self.rows, self.columns = shard.shape
        self.ring_rows = self.rows - shared
        self.cut = -(-max(self.ring_rows // 2, shared) // 16) * 16
        self.local = pltpu.make_async_copy(
            shard, full.at[rows_at(where.fsdp * self.rows, self.rows)], local_sem
        )
        far = where.far
        take = sems.take
        self.ring_sems = [[take() for _ in range(far)] for _ in range(2)]
        self.across_sems = [[take() for _ in range(far)] for _ in range(2)]
        self.twin_sems = [[take() for _ in range(far)] for _ in range(2)]
        self.twin_across_sems = [[take() for _ in range(far)] for _ in range(2)]
        self.build()

    def columns_of(self, core):
        half = self.columns // 2
        return pl.ds(pl.multiple_of(core * half, 128), half)

    def ring_span(self, direction, step):
        start, size = 0, self.ring_rows
        if step == self.where.far:
            start, size = (0, self.cut) if direction == 0 else (self.cut, self.ring_rows - self.cut)
        return start, size

    def ring_view(self, owner, direction, step, core, ref=None):
        start, size = self.ring_span(direction, step)
        start = start + self.where.plane * self.shared
        if ref is None:
            ref, start = self.full, start + owner * self.rows
        return ref.at[rows_at(start, size), self.columns_of(core)]

    def across_view(self, owner, plane, core):
        start = owner * self.rows + plane * (self.rows - self.shared)
        return self.full.at[rows_at(start, self.shared), self.columns_of(core)]

    def build(self):
        where, far = self.where, self.where.far
        near = range(1, far + 1)
        self.ring_out, self.ring_in, self.across_out, self.across_in = {}, {}, {}, {}
        self.twin_out, self.twin_in, self.twin_across_out, self.twin_across_in = {}, {}, {}, {}
        for direction in range(2):
            to = where.ring[direction]
            src = self.ring_view(None, direction, 1, where.core, self.shard)
            dst = self.ring_view(where.fsdp, direction, 1, where.core)
            self.ring_out[direction, 1] = remote(src, dst, self.ring_sems[direction][0], to)
            for step in near:
                owner = where.owner(direction, step)
                view = self.ring_view(owner, direction, step, where.core)
                self.ring_in[direction, step] = remote(view, view, self.ring_sems[direction][step - 1], to)
                sems = self.twin_sems[direction][step - 1]
                self.twin_out[direction, step] = remote(view, view, sems, where.twin)
                view = self.ring_view(owner, direction, step, 1 - where.core)
                self.twin_in[direction, step] = remote(view, view, sems, where.twin)
                if step < far:
                    view = self.ring_view(owner, direction, step + 1, where.core)
                    self.ring_out[direction, step + 1] = remote(view, view, self.ring_sems[direction][step], to)
                if step < far or direction == 0:
                    sems = self.across_sems[direction][step - 1]
                    view = self.across_view(owner, where.plane, where.core)
                    self.across_out[direction, step] = remote(view, view, sems, where.across)
                    view = self.across_view(owner, 1 - where.plane, where.core)
                    self.across_in[direction, step] = remote(view, view, sems, where.across)
                    sems = self.twin_across_sems[direction][step - 1]
                    self.twin_across_out[direction, step] = remote(view, view, sems, where.twin)
                    view = self.across_view(owner, 1 - where.plane, 1 - where.core)
                    self.twin_across_in[direction, step] = remote(view, view, sems, where.twin)

    def start(self):
        self.local.start()
        for direction in range(2):
            self.ring_out[direction, 1].start()

    def ring_step(self, step):
        far = self.where.far
        for direction in range(2):
            self.ring_in[direction, step].wait_recv()
            if step < far:
                self.ring_out[direction, step + 1].start()
                self.across_out[direction, step].start()
            self.twin_out[direction, step].start()
        if step == far:
            self.across_out[0, step].start()

    def across_step(self, step):
        for direction in range(2 if step < self.where.far else 1):
            self.across_in[direction, step].wait_recv()
            self.twin_across_out[direction, step].start()

    def tick(self, step):
        if step <= self.where.far:
            self.ring_step(step)
        if step > 1:
            self.across_step(step - 1)

    def finish(self):
        for table in (self.twin_in, self.twin_across_in):
            for copy in table.values():
                copy.wait_recv()
        self.local.wait()

    def drain(self):
        for table in (self.ring_out, self.across_out, self.twin_out, self.twin_across_out):
            for copy in table.values():
                copy.wait_send()


class Reduce:
    def __init__(self, where, sems, grad, out, shared, bufs):
        self.where, self.grad, self.out, self.shared = where, grad, out, shared
        self.pair, self.other, self.passing, self.final = bufs
        self.rows = self.pair.shape[0] // where.count
        self.half = self.pair.shape[1]
        self.ring_rows = self.rows - shared
        self.cut = -(-max(self.ring_rows // 2, shared) // 16) * 16
        far, count = where.far, where.count
        order = [(0, far)] + [(d, j) for j in range(far - 1, 0, -1) for d in range(2)] + [(0, 0)]
        self.owners = [self.target(*o) for o in order]
        theirs, mine = self.columns_of(1 - where.core), self.columns_of(where.core)
        self.mine = mine
        self.pair_out, self.other_out, self.other_in, self.ring_out, self.ring_in = [], [], [], {}, {}
        for owner in self.owners:
            rows = rows_at(owner * self.rows, self.rows)
            self.pair_out.append(remote(grad.at[rows, theirs], self.pair.at[rows], sems.take(), where.twin))
            give = rows_at(owner * self.rows + (1 - where.plane) * self.ring_rows, shared)
            came = self.other.at[rows_at(owner * shared, shared)]
            take = sems.take()
            self.other_out.append(remote(self.pair.at[give], came, take, where.across))
            self.other_in.append(remote(came, came, take, where.across))
        for direction in range(2):
            to = where.ring[direction]
            for step in range(1, far + 1):
                start, size = self.span(direction, step)
                rows = self.ring_rows_of(self.target(direction, far + 1 - step), start, size)
                came = self.passing.at[direction, step - 1, pl.ds(start, size)]
                take = sems.take()
                self.ring_out[direction, step] = remote(self.pair.at[rows], came, take, to)
                self.ring_in[direction, step] = remote(came, came, take, to)
        self.own = self.ring_rows_of(where.fsdp, 0, self.ring_rows)
        take = sems.take()
        self.final_out = remote(self.pair.at[self.own], self.final, take, where.across)
        self.final_in = remote(self.final, self.final, take, where.across)
        take = sems.take()
        given, taken = out.at[:, mine], out.at[:, theirs]
        self.out_out = remote(given, given, take, where.twin)
        self.out_in = remote(taken, taken, take, where.twin)

    @staticmethod
    def shapes(rows, columns, count, shared):
        half, ring_rows = columns // 2, rows - shared
        return [
            pltpu.VMEM((count * rows, half), jnp.bfloat16),
            pltpu.VMEM((count * shared, half), jnp.bfloat16),
            pltpu.VMEM((2, count // 2, ring_rows, half), jnp.bfloat16),
            pltpu.VMEM((ring_rows, half), jnp.bfloat16),
        ]

    @staticmethod
    def copies(count):
        return 2 * count + 2 * (count // 2) + 2

    def target(self, direction, distance):
        return self.where.owner(1 - direction, distance)

    def columns_of(self, core):
        return pl.ds(pl.multiple_of(core * self.half, 128), self.half)

    def span(self, direction, step):
        if step > 1:
            return 0, self.ring_rows
        return (0, self.cut) if direction == 0 else (self.cut, self.ring_rows - self.cut)

    def ring_rows_of(self, owner, start, size):
        return rows_at(owner * self.rows + self.where.plane * self.shared + start, size)

    def start(self):
        for copy in self.pair_out:
            copy.start()

    def add_pair(self, start=0, stop=None):
        for i in range(len(self.owners))[start:stop]:
            self.pair_out[i].wait_recv()
            rows = rows_at(self.owners[i] * self.rows, self.rows)
            self.pair[rows, :] = self.pair[rows, :] + self.grad[rows, self.mine]
            self.other_out[i].start()

    def sent_pair(self):
        for copy in self.pair_out:
            copy.wait_send()

    def add_other(self, start=0, stop=None):
        where = self.where
        for i in range(len(self.owners))[start:stop]:
            self.other_in[i].wait_recv()
            owner = self.owners[i]
            mine = rows_at(owner * self.rows + where.plane * self.ring_rows, self.shared)
            theirs = rows_at(owner * self.shared, self.shared)
            self.pair[mine, :] = self.pair[mine, :] + self.other[theirs, :]
            if i == 0:
                self.ring_send(1)

    def ring_send(self, step):
        for direction in range(2):
            self.ring_out[direction, step].start()

    def ring_step(self, step):
        far = self.where.far
        for direction in range(2):
            start, size = self.span(direction, step)
            self.ring_in[direction, step].wait_recv()
            if step < far:
                rows = self.ring_rows_of(self.target(direction, far - step), start, size)
                came = self.passing[direction, step - 1, pl.ds(start, size)]
                self.pair[rows, :] = self.pair[rows, :] + came
        if step < far:
            self.ring_send(step + 1)
            return
        total = self.pair[self.own, :].astype(jnp.float32)
        total = total + self.passing[0, step - 1].astype(jnp.float32)
        total = total + self.passing[1, step - 1].astype(jnp.float32)
        self.pair[self.own, :] = total.astype(jnp.bfloat16)
        self.final_out.start()

    def finish(self):
        where = self.where
        self.final_in.wait_recv()
        columns = self.mine
        plane, shared, ring_rows = where.plane, self.shared, self.ring_rows
        both = self.rows - 2 * shared
        base = where.fsdp * self.rows + plane * shared
        f32 = jnp.float32
        if both:
            mine = self.pair[rows_at(base + (1 - plane) * shared, both), :].astype(f32)
            theirs = self.final[rows_at(plane * shared, both), :].astype(f32)
            self.out[pl.ds(shared, both), columns] = mine + theirs
        mine = self.pair[rows_at(base + plane * (ring_rows - shared), shared), :]
        self.out[rows_at(plane * ring_rows, shared), columns] = mine.astype(f32)
        theirs = self.final[rows_at((1 - plane) * (ring_rows - shared), shared), :]
        self.out[rows_at((1 - plane) * ring_rows, shared), columns] = theirs.astype(f32)
        self.out_out.start()

    def close(self):
        self.out_in.wait_recv()
        for copy in self.other_out + list(self.ring_out.values()) + [self.final_out, self.out_out]:
            copy.wait_send()


SEG_ROWS = (1, 1, 3, 2, 1, 1, 1, 4, 1)
(G1, B1, QB, FR, OB, G2, B2, F1B, F2B) = range(9)
MLP = 3072


def offsets():
    starts, total = [], 0
    for m in SEG_ROWS:
        starts.append(total)
        total += m
    return starts, total


def unpack_small(slots, vec, count, seg):
    lane = lax.broadcasted_iota(jnp.int32, (1, 128), 1)
    starts, _ = offsets()
    for first, m in zip(starts, SEG_ROWS):
        pieces = [jnp.zeros((1, 128), jnp.float32) for _ in range(m * count * seg // 128)]
        for f in range(count):
            for i in range(m):
                at = (m * f + i) * seg
                v, s = at // 128, at % 128
                row = slots[f, first + i : first + i + 1, :]
                if s:
                    row = pltpu.roll(row, s, 1)
                pieces[v] = pieces[v] + jnp.where(lane >= s, row, 0.0)
                if s + seg > 128:
                    pieces[v + 1] = pieces[v + 1] + jnp.where(lane < s + seg - 128, row, 0.0)
        for v, piece in enumerate(pieces):
            at = first * count * seg + 128 * v
            vec[:, at : at + 128] = piece


def part_of(vec, which, start=0, size=None):
    starts, _ = offsets()
    base = starts[which] * D
    size = SEG_ROWS[which] * D if size is None else size
    return vec[:, base + start : base + start + size]


def half_swap(t):
    width = t.shape[-1]
    lane = lax.broadcasted_iota(jnp.int32, t.shape, 1)
    return jnp.where(lax.rem(lane, HD) < HD // 2, pltpu.roll(t, width - HD // 2, 1), pltpu.roll(t, HD // 2, 1))


def columns_down(ref, i):
    return jnp.broadcast_to(ref[i : i + 1, :], (128, 128)).T


def rope_tables(vec, col, row, cosine, sine, tables):
    step = lax.broadcasted_iota(jnp.int32, (32, D), 0).astype(jnp.float32)
    stacks = []
    for at in (0, D):
        angle = step * part_of(vec, FR, at, D)
        for table in (jnp.cos(angle), jnp.sin(angle)):
            high = table.astype(jnp.bfloat16)
            rest = table - high.astype(jnp.float32)
            middle = rest.astype(jnp.bfloat16)
            last = (rest - middle.astype(jnp.float32)).astype(jnp.bfloat16)
            stacks.append(jnp.concatenate([high, middle, last, jnp.zeros_like(high)], axis=0))
            tables[len(stacks) - 1] = stacks[-1]
    lane = lax.broadcasted_iota(jnp.int32, (128, 128), 1)
    slot = jnp.where(lane < 96, lax.rem(lane, 32), -1).astype(jnp.float32)
    wide = lax.broadcasted_iota(jnp.int32, (128, D), 1)
    sign = jnp.where(lax.rem(wide, HD) < HD // 2, -1.0, 1.0)
    for i in range(col.shape[0]):
        at = pl.ds(128 * i, 128)
        pick_col = jnp.where(columns_down(col, i) == slot, 1.0, 0.0).astype(jnp.bfloat16)
        pick_row = jnp.where(columns_down(row, i) == slot, 1.0, 0.0).astype(jnp.bfloat16)
        look = lambda pick, stack: jnp.dot(pick, stack, preferred_element_type=jnp.float32)
        cc, cs = look(pick_col, stacks[0]), look(pick_col, stacks[1])
        rc, rs = look(pick_row, stacks[2]), look(pick_row, stacks[3])
        cosine[at, :] = cc * rc - cs * rs
        sine[at, :] = (cs * rc + cc * rs) * sign


def image_bias(image, bias):
    for i in range(image.shape[0]):
        mine = columns_down(image, i)
        for j in range(image.shape[0]):
            same = mine == image[j : j + 1, :]
            bias[128 * i : 128 * i + 128, 128 * j : 128 * j + 128] = jnp.where(same, 0.0, MASKED)


def turn(source, target, start=0):
    def body(j):
        target[pl.ds(pl.multiple_of(start + 128 * j, 128), 128), :] = source[:, tile_at(j, 128)].T

    loop(source.shape[1] // 128, body)


def statistics(values):
    centre = values - jnp.mean(values, axis=-1, keepdims=True)
    spread = jnp.mean(centre * centre, axis=-1, keepdims=True)
    inverse = lax.rsqrt(spread + EPSILON)
    return centre * inverse, inverse


def loop(count, body):
    def run(i, carry):
        body(i)
        return carry

    lax.fori_loop(0, count, run, 0)


def tile_at(i, size):
    return pl.ds(pl.multiple_of(i * size, size), size)


def matmul(left, right):
    return jnp.dot(left, right, preferred_element_type=jnp.float32)


def matmul_nt(left, right):
    return lax.dot_general(left, right, (((1,), (1,)), ((), ())), preferred_element_type=jnp.float32)


def project(normed_low, weights, vec, cosine, sine, outs):
    tile = 256
    per = D // tile
    for which, out in enumerate(outs):
        def body(j, which=which, out=out):
            cols = tile_at(j, tile)
            wide = pl.ds(pl.multiple_of(which * D + j * tile, tile), tile)
            starts, _ = offsets()
            shift = vec[:, pl.ds(pl.multiple_of(starts[QB] * D + which * D + j * tile, tile), tile)]
            t = matmul(normed_low[...], weights[:, wide]) + shift
            if which < 2:
                t = t * cosine[:, cols] + half_swap(t) * sine[:, cols]
            if which == 0:
                t = t * HD**-0.5
            out[:, cols] = t.astype(jnp.bfloat16)

        loop(per, body)


def attend(pair, query, key, value, bias, mixed, lse, block):
    lane_all = lax.broadcasted_iota(jnp.int32, (1, 128), 1)
    cols = tile_at(pair, 128)
    lane = lax.broadcasted_iota(jnp.int32, (1, 128), 1)
    first = lane < HD
    k2, v2 = key[:, cols], value[:, cols]
    zero = jnp.zeros((), jnp.bfloat16)
    for start in range(0, query.shape[0], block):
        rows = pl.ds(start, block)
        q2 = query[rows, cols]
        total, sums, tops = None, [], []
        for keep in (first, ~first):
            s = matmul_nt(jnp.where(keep, q2, zero), k2) + bias[rows, :]
            top = jnp.max(s, axis=-1, keepdims=True)
            p = jnp.exp(s - top)
            sums.append(jnp.sum(p, axis=-1, keepdims=True))
            tops.append(top)
            o = matmul(p.astype(jnp.bfloat16), jnp.where(keep, v2, zero))
            total = o if total is None else total + o
        mixed[rows, cols] = (total / jnp.where(first, sums[0], sums[1])).astype(jnp.bfloat16)
        kept = lse[rows, :]
        for i in range(2):
            kept = jnp.where(lane_all == 2 * pair + i, tops[i] + jnp.log(sums[i]), kept)
        lse[rows, :] = kept


def norm_rows(source, normed_low, vec, gain, shift, block=128):
    def body(i):
        rows = tile_at(i, block)
        unit, _ = statistics(source[rows, :].astype(jnp.float32))
        normed_low[rows, :] = (unit * part_of(vec, gain) + part_of(vec, shift)).astype(jnp.bfloat16)

    loop(source.shape[0] // block, body)


def mix_out(x, mixed, weights, vec, middle):
    starts, _ = offsets()

    def body(j):
        cols = tile_at(j, 256)
        shift = vec[:, pl.ds(pl.multiple_of(starts[OB] * D + j * 256, 256), 256)]
        middle[:, cols] = x[:, cols].astype(jnp.float32) + matmul(mixed[...], weights[:, cols]) + shift

    loop(D // 256, body)


def hidden_tile(j, normed_low, weights, vec, active, active_t, slope):
    starts, _ = offsets()
    cols = tile_at(j, 256)
    shift = vec[:, pl.ds(pl.multiple_of(starts[F1B] * D + j * 256, 256), 256)]
    h = matmul(normed_low[...], weights[:, cols]) + shift
    c = (2.0 / math.pi) ** 0.5
    square = h * h
    t = jnp.tanh(c * h * (1.0 + 0.044715 * square))
    low = (0.5 * h * (1.0 + t)).astype(jnp.bfloat16)
    active[:, cols] = low
    active_t[cols, :] = low.T
    slope[:, cols] = (
        0.5 * (1.0 + t) + 0.5 * h * (1.0 - t * t) * (c * (1.0 + 3 * 0.044715 * square))
    ).astype(jnp.bfloat16)


def result_tile(j, middle, active, weights, vec, output):
    starts, _ = offsets()
    cols = tile_at(j, 256)
    shift = vec[:, pl.ds(pl.multiple_of(starts[F2B] * D + j * 256, 256), 256)]
    output[:, cols] = (middle[:, cols] + matmul(active[...], weights[:, cols]) + shift).astype(jnp.bfloat16)


def forward_kernel(count, seg, shares, *refs):
    (x, image, row, col, small, qkv_s, out_s, fc1_s, fc2_s) = refs[:9]
    (output, vec_o, tables_o, turned_o, q_o, k_o, v_o, lse_o, middle_o, act_t_o, slope_o,
     qkv_o, out_o, fc1_o, fc2_o) = refs[9:24]
    (slots, vec, tables, turned, q, k, v, lse_t, middle, act_t, slope, qkv_w, out_w, fc1_w, fc2_w,
     cosine, sine, bias, lse, act, low,
     send, recv, small_send, small_recv, local, saved) = refs[24:]
    n1 = mixed = n2 = low
    where = Place(count)
    peers = [(lax.rem(where.fsdp + i, count), where.dp) for i in range(1, count)]
    where.greet(peers)
    sems = Sems(send, recv)
    flows = [
        Gather(where, sems, s, w, shared, local.at[i])
        for i, (s, w, shared) in enumerate(
            zip((qkv_s, out_s, fc1_s, fc2_s), (qkv_w, out_w, fc1_w, fc2_w), shares)
        )
    ]
    qkv_f, out_f, fc1_f, fc2_f = flows
    far = where.far
    small_copies = [
        remote(small, slots.at[where.fsdp], (small_send.at[i], small_recv.at[i]), peers[i])
        for i in range(count - 1)
    ]
    for copy in small_copies:
        copy.start()
    qkv_f.start()
    out_f.start()
    slots[where.fsdp] = small[...]
    saves = []

    def save(source, target):
        copy = pltpu.make_async_copy(source, target, saved.at[len(saves)])
        copy.start()
        saves.append(copy)

    image_bias(image, bias)
    for i in range(1, count):
        came = slots.at[lax.rem(where.fsdp + count - i, count)]
        remote(came, came, (small_send.at[i - 1], small_recv.at[i - 1]), peers[i - 1]).wait_recv()
    unpack_small(slots, vec, count, seg)
    save(vec, vec_o)
    norm_rows(x, n1, vec, G1, B1)
    turn(n1, turned)
    qkv_f.tick(1)
    fc1_f.start()
    out_f.tick(1)
    rope_tables(vec, col, row, cosine, sine, tables)
    save(tables, tables_o)
    lse[...] = jnp.zeros_like(lse)
    for step in range(2, far + 2):
        qkv_f.tick(step)
        out_f.tick(step)
        if step == 3:
            fc2_f.start()
            fc1_f.tick(1)
    qkv_f.finish()
    project(n1, qkv_w, vec, cosine, sine, (q, k, v))
    out_f.finish()
    save(qkv_w, qkv_o)
    save(out_w, out_o)
    save(q, q_o)
    save(k, k_o)
    save(v, v_o)

    ticks = [(fc2_f, 1), (fc1_f, 2), (fc2_f, 2), (fc1_f, 3), (fc2_f, 3), (fc1_f, 4), (fc2_f, 4), (fc1_f, 5)]
    ticks = ticks if far == 4 else []

    def pair_body(j):
        attend(j, q, k, v, bias, mixed, lse, 320)
        for i, (flow, step) in enumerate(ticks):
            @pl.when(j == min(i // 2 + 1, 5))
            def _(flow=flow, step=step):
                flow.tick(step)

    loop(H // 2, pair_body)
    lse_t[...] = lse[...].T
    save(lse_t, lse_o)
    turn(mixed, turned, D)
    mix_out(x, mixed, out_w, vec, middle)
    save(middle, middle_o)
    norm_rows(middle, n2, vec, G2, B2)
    turn(n2, turned, 2 * D)
    save(turned, turned_o)
    fc2_f.tick(far + 1)
    fc1_f.finish()
    loop(MLP // 256, lambda j: hidden_tile(j, n2, fc1_w, vec, act, act_t, slope))
    save(act_t, act_t_o)
    save(slope, slope_o)
    save(fc1_w, fc1_o)
    fc2_f.finish()
    save(fc2_w, fc2_o)
    loop(D // 256, lambda j: result_tile(j, middle, act, fc2_w, vec, output))
    for flow in flows:
        flow.drain()
    for copy in small_copies:
        copy.wait_send()
    for copy in saves:
        copy.wait()


def forward(x, image, row, col, small, weights, count):
    bf16, f32 = jnp.bfloat16, jnp.float32
    tokens = x.shape[0]
    seg = D // count
    shares = tuple(w.shape[0] // 3 for w in weights)
    wide = lambda kind, width=D: ((tokens, width), kind)
    total = offsets()[1] * D
    full = [((w.shape[0] * count, w.shape[1]), bf16) for w in weights]
    kept = [
        ((1, total), f32), ((4, 128, D), bf16), ((3 * D, tokens), bf16), wide(bf16), wide(bf16), wide(bf16),
        ((128, tokens), f32), wide(f32), ((MLP, tokens), bf16), wide(bf16, MLP),
    ] + full
    copies = 4 * 8 * (count // 2)
    any_spec = pl.BlockSpec(memory_space=pl.ANY)
    vmem_spec = pl.BlockSpec(memory_space=pltpu.VMEM)
    scratch = kept + [
        wide(f32), wide(f32), ((tokens, tokens), f32), wide(f32, 128), wide(bf16, MLP), wide(bf16),
    ]
    return pl.pallas_call(
        partial(forward_kernel, count, seg, shares),
        out_shape=[jax.ShapeDtypeStruct((tokens, D), bf16)] + [jax.ShapeDtypeStruct(*s) for s in kept],
        in_specs=[vmem_spec] * 9,
        out_specs=[vmem_spec] + [any_spec] * len(kept),
        scratch_shapes=[pltpu.VMEM((count,) + small.shape, f32)]
        + [pltpu.VMEM(*s) for s in scratch]
        + [
            pltpu.SemaphoreType.DMA((copies,)),
            pltpu.SemaphoreType.DMA((copies,)),
            pltpu.SemaphoreType.DMA((count - 1,)),
            pltpu.SemaphoreType.DMA((count - 1,)),
            pltpu.SemaphoreType.DMA((4,)),
            pltpu.SemaphoreType.DMA((len(kept),)),
        ],
        compiler_params=pltpu.CompilerParams(
            collective_id=0, has_side_effects=True, vmem_limit_bytes=67043328
        ),
        name="forward",
    )(x, image, row, col, small, *weights)


def unit_and_inverse(source, rows):
    return statistics(source[rows, :].astype(jnp.float32))


def attend_back(pair, query, key, value, lse_t, bias, tables, pick_col, pick_row, colb, rowb, given, grads, sums, blocks):
    cols = tile_at(pair, 128)
    f32, bf16 = jnp.float32, jnp.bfloat16
    tokens = query.shape[0]
    lane = lax.broadcasted_iota(jnp.int32, (1, 128), 1)
    first = lane < HD
    zero = jnp.zeros((), bf16)
    q2, k2, v2, g2 = query[:, cols], key[:, cols], value[:, cols], given[:, cols]
    k2_t = k2.T
    grad_key = jnp.zeros((tokens, 128), f32)
    grad_value = jnp.zeros((tokens, 128), f32)
    turned = []
    for start, size in blocks:
        rows = slice(start, start + size)
        halves = []
        for i, keep in enumerate((first, ~first)):
            q1 = jnp.where(keep, q2[rows], zero)
            g1 = jnp.where(keep, g2[rows], zero)
            s = matmul_nt(k2, q1) + bias[:, rows]
            heads = lse_t[0:16, rows]
            head = lax.broadcasted_iota(jnp.int32, heads.shape, 0)
            p = jnp.exp(s - jnp.sum(jnp.where(head == 2 * pair + i, heads, 0.0), axis=0, keepdims=True))
            gp = matmul_nt(v2, g1)
            ds = p * (gp - jnp.sum(p * gp, axis=0, keepdims=True))
            ds = ds.astype(bf16)
            grad_value = grad_value + matmul(p.astype(bf16), g1)
            grad_key = grad_key + matmul(ds, q1)
            halves.append(matmul(k2_t[HD * i : HD * i + HD], ds))
        turned.append(jnp.concatenate(halves, axis=0).T)
    grad_query = jnp.concatenate(turned, axis=0) * HD**-0.5
    look = lambda pick, i: jnp.dot(pick[...], tables[i, :, cols], preferred_element_type=f32)
    cc, cs, rc, rs = look(pick_col, 0), look(pick_col, 1), look(pick_row, 2), look(pick_row, 3)
    sign = jnp.where(lax.rem(lane, HD) < HD // 2, -1.0, 1.0)
    cosine, sine = cc * rc - cs * rs, (cs * rc + cc * rs) * sign
    turn_sum = half_swap(q2.astype(f32)) * (grad_query * HD**0.5) + half_swap(k2.astype(f32)) * grad_key
    starts, _ = offsets()
    for i, where_at in enumerate((colb, rowb)):
        at = pl.ds(pl.multiple_of((starts[FR] + i) * D + 128 * pair, 128), 128)
        sums[:, at] = jnp.sum(turn_sum * where_at[...], axis=0, keepdims=True) * sign
    finals = (
        grad_query * cosine - half_swap(grad_query) * sine,
        grad_key * cosine - half_swap(grad_key) * sine,
        grad_value,
    )
    for i, final in enumerate(finals):
        low = final.astype(bf16)
        at = pl.ds(pl.multiple_of(i * D + 128 * pair, 128), 128)
        grads[:, at] = low
        at = pl.ds(pl.multiple_of((starts[QB] + i) * D + 128 * pair, 128), 128)
        sums[:, at] = jnp.sum(low.astype(f32), axis=0, keepdims=True)


def norm_back(source, grad, onward, gain, vec, sums, which_gain, which_shift, emit, block=128):
    starts, _ = offsets()
    gain_at = slice(starts[which_gain] * D, starts[which_gain] * D + D)
    shift_at = slice(starts[which_shift] * D, starts[which_shift] * D + D)
    sums[:, gain_at] = jnp.zeros((1, D), jnp.float32)
    sums[:, shift_at] = jnp.zeros((1, D), jnp.float32)

    def body(i):
        rows = tile_at(i, block)
        unit, inverse = statistics(source[rows, :].astype(jnp.float32))
        g = grad[rows, :]
        sums[:, gain_at] += jnp.sum(g * unit, axis=0, keepdims=True)
        sums[:, shift_at] += jnp.sum(g, axis=0, keepdims=True)
        e = g * part_of(vec, gain)
        mean = jnp.mean(e, axis=-1, keepdims=True)
        along = jnp.mean(e * unit, axis=-1, keepdims=True)
        emit(rows, onward[rows, :].astype(jnp.float32) + inverse * (e - mean - unit * along))

    loop(source.shape[0] // block, body)


def pack_sums(sums, slots, count, seg):
    lane = lax.broadcasted_iota(jnp.int32, (1, 128), 1)
    starts, _ = offsets()
    slots[...] = jnp.zeros_like(slots)
    for first, m in zip(starts, SEG_ROWS):
        for f in range(count):
            for i in range(m):
                at = first * count * seg + (m * f + i) * seg
                v, s = at // 128, at % 128
                row = sums[:, 128 * v : 128 * v + 128]
                if s:
                    row = pltpu.roll(row, 128 - s, 1)
                if s + seg > 128:
                    more = pltpu.roll(sums[:, 128 * v + 128 : 128 * v + 256], 128 - s, 1)
                    row = jnp.where(lane < 128 - s, row, more)
                slots[f, first + i : first + i + 1, :] = jnp.where(lane < seg, row, 0.0)


def backward_kernel(count, seg, shared, wide_shared, *refs):
    (x, grad_out, image, row, col, vec_h, tables_h, turned_h, q_h, k_h, v_h, lse_h, middle_h, act_t_h, slope_h,
     qkv_h, out_h, fc1_h, fc2_h) = refs[:19]
    (grad_x, small_out, grad_qkv, grad_out_w, grad_fc1, grad_fc2) = refs[19:25]
    (vec, tables, q, k, v, lse_t, middle, act_t, slope, out_w, fc1_w, fc2_w,
     bias, pick_col, pick_row, colb, rowb, wide, low, big, sums, slots, slots_twin, slots_across, slots_in) = refs[25:50]
    outs = refs[50:57]
    bufs = refs[57:93]
    send, recv, small_send, small_recv, loaded = refs[93:]
    f32, bf16 = jnp.float32, jnp.bfloat16
    where = Place(count)
    far = where.far
    starts, _ = offsets()

    loads = {}

    def load(name, source, target):
        copy = pltpu.make_async_copy(source, target, loaded.at[len(loads)])
        copy.start()
        loads[name] = copy

    load("act", act_t_h, act_t)
    load("fc2", fc2_h, fc2_w)
    load("slope", slope_h, slope)
    load("fc1", fc1_h, fc1_w)
    for name, source, target in (
        ("vec", vec_h, vec), ("middle", middle_h, middle), ("out", out_h, out_w), ("q", q_h, q), ("k", k_h, k),
        ("v", v_h, v), ("lse", lse_h, lse_t), ("tables", tables_h, tables),
    ):
        load(name, source, target)
    peers = [(lax.rem(where.fsdp + i, count), where.dp) for i in range(1, count)]
    where.greet(peers)
    sems = Sems(send, recv)
    fc2 = Reduce(where, sems, big, grad_fc2, wide_shared, bufs[:4])
    parts = [
        Reduce(
            where, sems, big.at[pl.ds(D * (i % 4), D)], grad_out_w if i == 4 else outs[i - (i > 4)],
            shared, bufs[4 + 4 * i : 8 + 4 * i],
        )
        for i in range(8)
    ]

    loads["act"].wait()
    loop(8, lambda i: store_tile(big, i, 384, act_t, grad_out))
    fc2.start()
    at = starts[F2B] * D
    sums[:, at : at + D] = jnp.sum(grad_out[...].astype(f32), axis=0, keepdims=True)
    loads["fc2"].wait()
    loads["slope"].wait()
    load("turned", turned_h, act_t.at[pl.ds(0, 3 * D)])
    normed_one, mixed_t, normed_two = (act_t.at[pl.ds(D * i, D)] for i in range(3))

    def hidden(j):
        cols = tile_at(j, 256)
        g = matmul_nt(grad_out[...], fc2_w[cols, :]) * slope[:, cols].astype(f32)
        g = g.astype(bf16)
        slope[:, cols] = g
        at = pl.ds(pl.multiple_of(starts[F1B] * D + 256 * j, 256), 256)
        sums[:, at] = jnp.sum(g.astype(f32), axis=0, keepdims=True)

    loop(MLP // 256, hidden)
    fc2.add_pair()
    fc2.sent_pair()
    loads["turned"].wait()
    for i in range(4):
        grad_part = slope.at[:, pl.ds(D * i, D)]
        loop(2, lambda j: store_tile(big.at[pl.ds(D * i, D)], j, 384, normed_two, grad_part))
        parts[i].start()
        if i:
            parts[i - 1].add_pair()
        if i == 1:
            fc2.add_other()
        if i == 3:
            fc2.ring_step(1)
    loads["fc1"].wait()

    def normed_grad(j):
        cols = tile_at(j, 256)
        wide[:, cols] = matmul_nt(slope[...], fc1_w[cols, :])

    normed_grad(0)
    parts[3].add_pair()
    parts[0].add_other()
    normed_grad(1)
    parts[1].add_other()
    fc2.ring_step(2)
    parts[0].ring_step(1)
    normed_grad(2)
    for i in range(4):
        parts[i].sent_pair()
    load("qkv", qkv_h, big_rows(fc1_w))
    loads["vec"].wait()
    loads["middle"].wait()
    parts[2].add_other()
    parts[1].ring_step(1)

    at = starts[OB] * D
    sums[:, at : at + D] = jnp.zeros((1, D), f32)

    def keep_middle(rows, total):
        wide[rows, :] = total
        total = total.astype(bf16)
        low[rows, :] = total
        sums[:, at : at + D] += jnp.sum(total.astype(f32), axis=0, keepdims=True)

    norm_back(middle, wide, grad_out, G2, vec, sums, G2, B2, keep_middle)
    parts[3].add_other()
    fc2.ring_step(3)
    parts[0].ring_step(2)
    parts[2].ring_step(1)
    loop(2, lambda j: store_tile(big.at[pl.ds(0, D)], j, 384, mixed_t, low))
    parts[4].start()
    loads["out"].wait()
    mixed_grad = slope.at[:, pl.ds(3 * D, D)]

    def mix_back(j):
        cols = tile_at(j, 256)
        mixed_grad[:, cols] = matmul_nt(low[...], out_w[cols, :]).astype(bf16)

    loop(D // 256, mix_back)
    parts[4].add_pair()

    image_bias(image, bias)
    lane = lax.broadcasted_iota(jnp.int32, (128, 128), 1)
    slot = jnp.where(lane < 96, lax.rem(lane, 32), -1).astype(f32)
    for i in range(col.shape[0]):
        rows = slice(128 * i, 128 * i + 128)
        for source, kept, pick in ((col, colb, pick_col), (row, rowb, pick_row)):
            down = columns_down(source, i)
            kept[rows, :] = down
            pick[rows, :] = jnp.where(down == slot, 1.0, 0.0).astype(bf16)
    for name in ("q", "k", "v", "lse", "tables"):
        loads[name].wait()

    turns = {
        0: [lambda: parts[3].ring_step(1), lambda: fc2.ring_step(4), lambda: parts[0].ring_step(3),
            lambda: parts[1].ring_step(2), lambda: parts[4].add_other()],
        1: [lambda: parts[2].ring_step(2), lambda: parts[0].ring_step(4), lambda: parts[3].ring_step(2),
            lambda: parts[1].ring_step(3), lambda: parts[4].ring_step(1)],
        2: [lambda: fc2.finish(), lambda: parts[2].ring_step(3), lambda: parts[1].ring_step(4),
            lambda: parts[3].ring_step(3), lambda: parts[4].ring_step(2), lambda: parts[5].add_pair()],
        3: [lambda: parts[0].finish(), lambda: parts[2].ring_step(4), lambda: parts[3].ring_step(4),
            lambda: parts[4].ring_step(3), lambda: parts[5].add_other()],
        4: [lambda: parts[1].finish(), lambda: parts[4].ring_step(4), lambda: parts[5].ring_step(1),
            lambda: parts[6].add_pair()],
        5: [lambda: parts[2].finish(), lambda: parts[5].ring_step(2), lambda: parts[6].add_other()],
    }
    tokens = q.shape[0]
    blocks = [(i, min(256, tokens - i)) for i in range(0, tokens, 256)]

    def pair_body(j):
        attend_back(
            j, q, k, v, lse_t, bias, tables, pick_col, pick_row, colb, rowb, mixed_grad, slope, sums, blocks
        )
        for i, steps in turns.items():
            @pl.when(j == i)
            def _(i=i, steps=steps):
                if i % 2:
                    project_back(parts[5 + i // 2].grad, normed_one, slope, i // 2)
                    parts[5 + i // 2].start()
                for step in steps:
                    step()

    loop(H // 2, pair_body)
    loads["qkv"].wait()
    qkv_w = big_rows(fc1_w)
    parts[7].add_pair()
    parts[5].ring_step(3)
    parts[6].ring_step(1)

    def normed_one_grad(j):
        cols = tile_at(j, 256)
        middle[:, cols] = matmul_nt(slope[:, pl.ds(0, 3 * D)], qkv_w[cols, :])

    normed_one_grad(0)
    parts[7].add_other()
    parts[5].ring_step(4)
    parts[6].ring_step(2)
    normed_one_grad(1)
    parts[7].ring_step(1)
    parts[6].ring_step(3)
    parts[3].finish()
    normed_one_grad(2)
    parts[7].ring_step(2)
    parts[6].ring_step(4)
    parts[4].finish()

    def keep_x(rows, total):
        grad_x[rows, :] = total.astype(bf16)

    norm_back(x, middle, wide, G1, vec, sums, G1, B1, keep_x)
    parts[7].ring_step(3)
    pack_sums(sums, slots, count, seg)
    take = lambda i: (small_send.at[i], small_recv.at[i])
    to_twin = remote(slots, slots_twin, take(0), where.twin)
    to_twin.start()
    parts[5].finish()
    parts[7].ring_step(4)
    to_twin.wait()
    slots[...] = slots[...] + slots_twin[...]
    to_across = remote(slots, slots_across, take(1), where.across)
    to_across.start()
    parts[6].finish()
    to_across.wait()
    slots[...] = slots[...] + slots_across[...]
    slots_in[where.fsdp] = slots[where.fsdp]
    given = [
        remote(slots.at[peer[0]], slots_in.at[where.fsdp], take(2 + i), peer) for i, peer in enumerate(peers)
    ]
    for copy in given:
        copy.start()
    parts[7].finish()
    for i in range(1, count):
        came = slots_in.at[lax.rem(where.fsdp + count - i, count)]
        remote(came, came, take(1 + i), peers[i - 1]).wait_recv()
    total = slots_in[0]
    for i in range(1, count):
        total = total + slots_in[i]
    small_out[...] = total
    for copy in given:
        copy.wait_send()
    for i in range(4, 8):
        parts[i].sent_pair()
    fc2.close()
    for part in parts:
        part.close()
    for i in range(4):
        grad_fc1[:, pl.ds(D * i, D)] = outs[i][...]
    for m in range(3):
        for i in range(3):
            grad_qkv[:, pl.ds(i * D + 256 * m, 256)] = outs[4 + m][:, pl.ds(256 * i, 256)]


def store_tile(target, i, size, left, right):
    rows = tile_at(i, size)
    target[rows, :] = matmul(left[rows, :], right[...]).astype(jnp.bfloat16)


def big_rows(ref):
    return ref.at[:, pl.ds(0, 3 * D)]


def project_back(target, normed, grads, m):
    for i in range(3):
        target[:, pl.ds(256 * i, 256)] = matmul(normed[...], grads[:, pl.ds(i * D + 256 * m, 256)]).astype(jnp.bfloat16)


def backward(x, grad_out, image, row, col, kept, count):
    bf16, f32 = jnp.bfloat16, jnp.float32
    tokens = x.shape[0]
    seg = D // count
    shared, wide_shared = seg // 96 * 16, seg
    (vec, tables, turned, q, k, v, lse, middle, act_t, slope, qkv, out, fc1, fc2) = kept
    like = lambda a: pltpu.VMEM(a.shape, a.dtype)
    side = pltpu.VMEM((tokens, 128), f32)
    pick = pltpu.VMEM((tokens, 128), bf16)
    slots = pltpu.VMEM((count, 16, 128), f32)
    part = pltpu.VMEM((seg, D), f32)
    flows = Reduce.shapes(MLP // count, D, count, wide_shared)
    for _ in range(8):
        flows = flows + Reduce.shapes(seg, D, count, shared)
    copies = 9 * Reduce.copies(count)
    any_spec = pl.BlockSpec(memory_space=pl.ANY)
    vmem_spec = pl.BlockSpec(memory_space=pltpu.VMEM)
    dma = pltpu.SemaphoreType.DMA
    return pl.pallas_call(
        partial(backward_kernel, count, seg, shared, wide_shared),
        out_shape=[
            jax.ShapeDtypeStruct((tokens, D), bf16),
            jax.ShapeDtypeStruct((16, 128), f32),
            jax.ShapeDtypeStruct((seg, 3 * D), f32),
            jax.ShapeDtypeStruct((seg, D), f32),
            jax.ShapeDtypeStruct((seg, MLP), f32),
            jax.ShapeDtypeStruct((MLP // count, D), f32),
        ],
        in_specs=[vmem_spec] * 5 + [any_spec] * len(kept),
        out_specs=[vmem_spec] * 6,
        scratch_shapes=[like(a) for a in (vec, tables, q, k, v, lse, middle, act_t, slope, out, fc1, fc2)]
        + [
            pltpu.VMEM((tokens, tokens), f32), pick, pick, side, side,
            pltpu.VMEM((tokens, D), f32), pltpu.VMEM((tokens, D), bf16), pltpu.VMEM((MLP, D), bf16),
            pltpu.VMEM(vec.shape, f32), slots, slots, slots, slots,
        ]
        + [part] * 7
        + flows
        + [dma((copies,)), dma((copies,)), dma((count + 1,)), dma((count + 1,)), dma((len(kept),))],
        compiler_params=pltpu.CompilerParams(
            collective_id=1, has_side_effects=True, vmem_limit_bytes=67043328
        ),
        name="backward",
    )(x, grad_out, image, row, col, *kept)


def pack_small(parts, count):
    seg = D // count
    rows = []
    for i, part in enumerate(parts):
        if i == FR:
            part = jnp.broadcast_to(part.reshape(-1, 1, HD // 2), (seg // (HD // 2), 2, HD // 2))
        rows.append(part.reshape(-1, seg))
    rows = jnp.concatenate(rows, axis=0).astype(jnp.float32)
    return jnp.pad(rows, ((0, -rows.shape[0] % 8), (0, 128 - seg)))


def normed(values, scales, shifts):
    centre = values - jnp.mean(values, axis=-1, keepdims=True)
    spread = jnp.mean(centre * centre, axis=-1, keepdims=True)
    return centre * lax.rsqrt(spread + EPSILON) * scales + shifts


def rotate(queries, keys_in, frequency, row_pos, col_pos):
    half_dim = queries.shape[-1] // 2
    head_count = queries.shape[1]
    split_at = head_count * half_dim
    along_col = frequency[:split_at].reshape(head_count, half_dim)
    along_row = frequency[split_at:].reshape(head_count, half_dim)
    angles = col_pos[:, None, None] * along_col[None] + row_pos[:, None, None] * along_row[None]
    cosine = jnp.cos(angles)
    sine_part = jnp.sin(angles)

    def turned(operand):
        first_half = operand[..., :half_dim]
        second_half = operand[..., half_dim:]
        return jnp.concatenate(
            [
                first_half * cosine - second_half * sine_part,
                first_half * sine_part + second_half * cosine,
            ],
            axis=-1,
        )

    return (turned(queries), turned(keys_in))


def body(
    layer_in,
    ln1_gain,
    ln1_bias,
    qkv_weight,
    qkv_bias,
    rope_freqs,
    out_weight,
    out_bias,
    ln2_gain,
    ln2_bias,
    fc1_weight,
    fc1_bias,
    fc2_weight,
    fc2_bias,
    image_of,
    patch_row,
    patch_col,
    grad_out,
):
    gathered = (
        lax.all_gather(ln1_gain, "fsdp", axis=0, tiled=True),
        lax.all_gather(ln1_bias, "fsdp", axis=0, tiled=True),
        lax.all_gather(qkv_weight, "fsdp", axis=0, tiled=True),
        lax.all_gather(qkv_bias, "fsdp", axis=0, tiled=True),
        lax.all_gather(rope_freqs, "fsdp", axis=0, tiled=True),
        lax.all_gather(out_weight, "fsdp", axis=0, tiled=True),
        lax.all_gather(out_bias, "fsdp", axis=0, tiled=True),
        lax.all_gather(ln2_gain, "fsdp", axis=0, tiled=True),
        lax.all_gather(ln2_bias, "fsdp", axis=0, tiled=True),
        lax.all_gather(fc1_weight, "fsdp", axis=0, tiled=True),
        lax.all_gather(fc1_bias, "fsdp", axis=0, tiled=True),
        lax.all_gather(fc2_weight, "fsdp", axis=0, tiled=True),
        lax.all_gather(fc2_bias, "fsdp", axis=0, tiled=True),
    )
    (
        gain_one,
        shift_one,
        qkv_mat,
        qkv_shift,
        frequency,
        out_mat,
        out_shift,
        gain_two,
        shift_two,
        fc1_mat,
        fc1_shift,
        fc2_mat,
        fc2_shift,
    ) = gathered
    token_count = layer_in.shape[0]
    inputs = layer_in.astype(jnp.float32)
    row_pos = patch_row.astype(jnp.float32)
    col_pos = patch_col.astype(jnp.float32)
    scale_qk = HD ** (-0.5)
    same_image = image_of[:, None] == image_of[None, :]
    normed_one, norm_one_pull = jax.vjp(
        normed, inputs, gain_one.astype(jnp.float32), shift_one.astype(jnp.float32)
    )
    normed_one_low = normed_one.astype(jnp.bfloat16)
    projected = jnp.dot(
        normed_one_low, qkv_mat, preferred_element_type=jnp.float32
    ) + qkv_shift.astype(jnp.float32)
    queries = projected[:, :D].reshape(token_count, H, HD)
    keys_in = projected[:, D : 2 * D].reshape(token_count, H, HD)
    values_in = projected[:, 2 * D :].reshape(token_count, H, HD)
    rotation = partial(rotate, row_pos=row_pos, col_pos=col_pos)
    (query_rot, key_rot), rope_pull = jax.vjp(
        rotation, queries, keys_in, frequency.astype(jnp.float32)
    )
    query_heads = query_rot.astype(jnp.bfloat16).transpose(1, 0, 2)
    key_heads = key_rot.astype(jnp.bfloat16).transpose(1, 0, 2)
    value_heads = values_in.astype(jnp.bfloat16).transpose(1, 0, 2)

    def head_scores(query_one, key_one):
        scores = (
            jnp.einsum("qd,kd->qk", query_one, key_one, preferred_element_type=jnp.float32)
            * scale_qk
        )
        return jnp.where(same_image, scores, MASKED)

    def head_forward(operands):
        query_one, key_one, value_one = operands
        scores = head_scores(query_one, key_one)
        peak_score = jnp.max(scores, axis=-1, keepdims=True)
        log_total = peak_score + jnp.log(
            jnp.sum(jnp.exp(scores - peak_score), axis=-1, keepdims=True)
        )
        probs = jnp.exp(scores - log_total)
        mixed_one = jnp.dot(
            probs.astype(jnp.bfloat16), value_one, preferred_element_type=jnp.float32
        )
        return (mixed_one, log_total[:, 0])

    mixed_heads, log_totals = lax.map(head_forward, (query_heads, key_heads, value_heads))
    mixed_low = mixed_heads.transpose(1, 0, 2).reshape(token_count, D).astype(jnp.bfloat16)
    middle = (
        inputs
        + jnp.dot(mixed_low, out_mat, preferred_element_type=jnp.float32)
        + out_shift.astype(jnp.float32)
    )
    normed_two, norm_two_pull = jax.vjp(
        normed, middle, gain_two.astype(jnp.float32), shift_two.astype(jnp.float32)
    )
    normed_two_low = normed_two.astype(jnp.bfloat16)
    hidden = jnp.dot(
        normed_two_low, fc1_mat, preferred_element_type=jnp.float32
    ) + fc1_shift.astype(jnp.float32)
    active, gelu_pull = jax.vjp(jax.nn.gelu, hidden)
    active_low = active.astype(jnp.bfloat16)
    result = (
        middle
        + jnp.dot(active_low, fc2_mat, preferred_element_type=jnp.float32)
        + fc2_shift.astype(jnp.float32)
    )
    output = result.astype(jnp.bfloat16)
    again = (
        lax.all_gather(ln1_gain, "fsdp", axis=0, tiled=True),
        lax.all_gather(ln1_bias, "fsdp", axis=0, tiled=True),
        lax.all_gather(qkv_weight, "fsdp", axis=0, tiled=True),
        lax.all_gather(qkv_bias, "fsdp", axis=0, tiled=True),
        lax.all_gather(rope_freqs, "fsdp", axis=0, tiled=True),
        lax.all_gather(out_weight, "fsdp", axis=0, tiled=True),
        lax.all_gather(out_bias, "fsdp", axis=0, tiled=True),
        lax.all_gather(ln2_gain, "fsdp", axis=0, tiled=True),
        lax.all_gather(ln2_bias, "fsdp", axis=0, tiled=True),
        lax.all_gather(fc1_weight, "fsdp", axis=0, tiled=True),
        lax.all_gather(fc1_bias, "fsdp", axis=0, tiled=True),
        lax.all_gather(fc2_weight, "fsdp", axis=0, tiled=True),
        lax.all_gather(fc2_bias, "fsdp", axis=0, tiled=True),
    )
    qkv_back = again[2]
    out_back = again[5]
    fc1_back = again[9]
    fc2_back = again[11]
    upstream = grad_out.astype(jnp.float32)
    grad_fc2 = jnp.einsum("ti,to->io", active_low, grad_out, preferred_element_type=jnp.float32)
    grad_fc2_shift = jnp.sum(upstream, axis=0)
    grad_active = jnp.einsum("to,io->ti", grad_out, fc2_back, preferred_element_type=jnp.float32)
    (grad_hidden,) = gelu_pull(grad_active)
    grad_hidden_low = grad_hidden.astype(jnp.bfloat16)
    grad_fc1 = jnp.einsum(
        "td,th->dh", normed_two_low, grad_hidden_low, preferred_element_type=jnp.float32
    )
    grad_fc1_shift = jnp.sum(grad_hidden_low.astype(jnp.float32), axis=0)
    grad_normed_two = jnp.einsum(
        "th,dh->td", grad_hidden_low, fc1_back, preferred_element_type=jnp.float32
    )
    grad_middle_norm, grad_gain_two, grad_shift_two = norm_two_pull(grad_normed_two)
    grad_middle = upstream + grad_middle_norm
    grad_middle_low = grad_middle.astype(jnp.bfloat16)
    grad_out_shift = jnp.sum(grad_middle_low.astype(jnp.float32), axis=0)
    grad_out_mat = jnp.einsum(
        "ti,to->io", mixed_low, grad_middle_low, preferred_element_type=jnp.float32
    )
    grad_mixed = jnp.einsum(
        "to,io->ti", grad_middle_low, out_back, preferred_element_type=jnp.float32
    )
    grad_mixed_heads = (
        grad_mixed.astype(jnp.bfloat16).reshape(token_count, H, HD).transpose(1, 0, 2)
    )

    def head_backward(operands):
        query_one, key_one, value_one, grad_one, log_total = operands
        scores = head_scores(query_one, key_one)
        probs = jnp.exp(scores - log_total[:, None])
        grad_value = jnp.einsum(
            "qk,qd->kd", probs.astype(jnp.bfloat16), grad_one, preferred_element_type=jnp.float32
        )
        grad_probs = jnp.einsum(
            "qd,kd->qk", grad_one, value_one, preferred_element_type=jnp.float32
        )
        grad_scores = probs * (grad_probs - jnp.sum(probs * grad_probs, axis=-1, keepdims=True))
        grad_scores_low = grad_scores.astype(jnp.bfloat16)
        grad_query = (
            jnp.einsum("qk,kd->qd", grad_scores_low, key_one, preferred_element_type=jnp.float32)
            * scale_qk
        )
        grad_key = (
            jnp.einsum("qk,qd->kd", grad_scores_low, query_one, preferred_element_type=jnp.float32)
            * scale_qk
        )
        return (grad_query, grad_key, grad_value)

    grad_query_heads, grad_key_heads, grad_value_heads = lax.map(
        head_backward, (query_heads, key_heads, value_heads, grad_mixed_heads, log_totals)
    )
    grad_query_rot = grad_query_heads.transpose(1, 0, 2)
    grad_key_rot = grad_key_heads.transpose(1, 0, 2)
    grad_values = grad_value_heads.transpose(1, 0, 2)
    grad_queries, grad_keys, grad_frequency = rope_pull((grad_query_rot, grad_key_rot))
    grad_projected = jnp.concatenate(
        [
            grad_queries.reshape(token_count, D),
            grad_keys.reshape(token_count, D),
            grad_values.reshape(token_count, D),
        ],
        axis=1,
    ).astype(jnp.bfloat16)
    grad_qkv_shift = jnp.sum(grad_projected.astype(jnp.float32), axis=0)
    grad_qkv = jnp.einsum(
        "td,tp->dp", normed_one_low, grad_projected, preferred_element_type=jnp.float32
    )
    grad_normed_one = jnp.einsum(
        "tp,dp->td", grad_projected, qkv_back, preferred_element_type=jnp.float32
    )
    grad_input_norm, grad_gain_one, grad_shift_one = norm_one_pull(grad_normed_one)
    grad_x = (grad_middle + grad_input_norm).astype(jnp.bfloat16)
    owned = (
        lax.psum_scatter(grad_gain_one, "fsdp", scatter_dimension=0, tiled=True),
        lax.psum_scatter(grad_shift_one, "fsdp", scatter_dimension=0, tiled=True),
        lax.psum_scatter(grad_qkv, "fsdp", scatter_dimension=0, tiled=True),
        lax.psum_scatter(grad_qkv_shift, "fsdp", scatter_dimension=0, tiled=True),
        lax.psum_scatter(grad_frequency, "fsdp", scatter_dimension=0, tiled=True),
        lax.psum_scatter(grad_out_mat, "fsdp", scatter_dimension=0, tiled=True),
        lax.psum_scatter(grad_out_shift, "fsdp", scatter_dimension=0, tiled=True),
        lax.psum_scatter(grad_gain_two, "fsdp", scatter_dimension=0, tiled=True),
        lax.psum_scatter(grad_shift_two, "fsdp", scatter_dimension=0, tiled=True),
        lax.psum_scatter(grad_fc1, "fsdp", scatter_dimension=0, tiled=True),
        lax.psum_scatter(grad_fc1_shift, "fsdp", scatter_dimension=0, tiled=True),
        lax.psum_scatter(grad_fc2, "fsdp", scatter_dimension=0, tiled=True),
        lax.psum_scatter(grad_fc2_shift, "fsdp", scatter_dimension=0, tiled=True),
    )
    summed = lax.psum(
        (
            owned[0],
            owned[1],
            owned[2],
            owned[3],
            owned[4],
            owned[5],
            owned[6],
            owned[7],
            owned[8],
            owned[9],
            owned[10],
            owned[11],
            owned[12],
        ),
        "dp",
    )
    return (
        output,
        grad_x,
        summed[0],
        summed[1],
        summed[2],
        summed[3],
        summed[4],
        summed[5],
        summed[6],
        summed[7],
        summed[8],
        summed[9],
        summed[10],
        summed[11],
        summed[12],
    )


def fast_body(
    layer_in,
    ln1_gain,
    ln1_bias,
    qkv_weight,
    qkv_bias,
    rope_freqs,
    out_weight,
    out_bias,
    ln2_gain,
    ln2_bias,
    fc1_weight,
    fc1_bias,
    fc2_weight,
    fc2_bias,
    image_of,
    patch_row,
    patch_col,
    grad_out,
):
    count = lax.axis_size("fsdp")
    seg = D // count
    parts = (ln1_gain, ln1_bias, qkv_bias, rope_freqs, out_bias, ln2_gain, ln2_bias, fc1_bias, fc2_bias)
    small = pack_small(parts, count)
    image, row, col = (a.reshape(-1, 128).astype(jnp.float32) for a in (image_of, patch_row, patch_col))
    output, *kept = forward(
        layer_in, image, row, col, small, (qkv_weight, out_weight, fc1_weight, fc2_weight), count
    )
    grad_x, sums, grad_qkv, grad_out_w, grad_fc1, grad_fc2 = backward(
        layer_in, grad_out, image, row, col, kept, count
    )
    starts, _ = offsets()
    owned = [sums[s : s + m, :seg].reshape(-1) for s, m in zip(starts, SEG_ROWS)]
    owned[FR] = owned[FR].reshape(-1, 2, HD // 2).sum(axis=1).reshape(-1)
    return (
        output,
        grad_x,
        owned[G1],
        owned[B1],
        grad_qkv,
        owned[QB],
        owned[FR],
        grad_out_w,
        owned[OB],
        owned[G2],
        owned[B2],
        grad_fc1,
        owned[F1B],
        grad_fc2,
        owned[F2B],
    )


def fits(mesh, tokens):
    count, planes = mesh.shape["fsdp"], mesh.shape["dp"]
    return count == 8 and planes == 4 and tokens == 640 * count * planes


def solution(mesh):
    in_specs = (
        P(("fsdp", "dp"), None),
        P("fsdp"),
        P("fsdp"),
        P("fsdp", None),
        P("fsdp"),
        P("fsdp"),
        P("fsdp", None),
        P("fsdp"),
        P("fsdp"),
        P("fsdp"),
        P("fsdp", None),
        P("fsdp"),
        P("fsdp", None),
        P("fsdp"),
        P(("fsdp", "dp")),
        P(("fsdp", "dp")),
        P(("fsdp", "dp")),
        P(("fsdp", "dp"), None),
    )
    out_specs = (
        P(("fsdp", "dp"), None),
        P(("fsdp", "dp"), None),
        P("fsdp"),
        P("fsdp"),
        P("fsdp", None),
        P("fsdp"),
        P("fsdp"),
        P("fsdp", None),
        P("fsdp"),
        P("fsdp"),
        P("fsdp"),
        P("fsdp", None),
        P("fsdp"),
        P("fsdp", None),
        P("fsdp"),
    )
    def step(*arguments):
        chosen = fast_body if fits(mesh, arguments[0].shape[0]) else body
        mapped = jax.shard_map(chosen, mesh=mesh, in_specs=in_specs, out_specs=out_specs, check_vma=False)
        return mapped(*arguments)

    return step
```

```python
import math
from functools import partial

import jax
import jax.numpy as jnp
from jax import lax
from jax.experimental import pallas as pl
from jax.experimental.pallas import tpu as pltpu
from jax.sharding import PartitionSpec as P

D = 768
H = 12
HD = 64
EPSILON = 1e-06
MASKED = -1e30

MESH = pl.DeviceIdType.MESH


def position(index, count):
    odd = lax.rem(index, 2)
    half = lax.div(index, 2)
    return (1 - odd) * half + odd * (count - 1 - half)


def member(place, count):
    place = lax.rem(place + 2 * count, count)
    back = lax.div(place, count // 2)
    return (1 - back) * 2 * place + back * (2 * (count - 1 - place) + 1)


class Place:
    def __init__(self, count):
        self.count = count
        self.far = count // 2
        self.fsdp = lax.axis_index("fsdp")
        self.dp = lax.axis_index("dp")
        self.plane = lax.div(self.dp, 2)
        self.core = lax.rem(self.dp, 2)
        self.place = position(self.fsdp, count)
        self.ring = (
            (member(self.place + 1, count), self.dp),
            (member(self.place - 1, count), self.dp),
        )
        self.across = (self.fsdp, (1 - self.plane) * 2 + self.core)
        self.twin = (self.fsdp, self.plane * 2 + 1 - self.core)

    def owner(self, direction, step):
        return member(self.place - step if direction == 0 else self.place + step, self.count)

    def greet(self, peers=None):
        barrier = pltpu.get_barrier_semaphore()
        partners = tuple(self.ring if peers is None else peers) + (self.across, self.twin)
        for device in partners:
            pl.semaphore_signal(barrier, inc=1, device_id=device, device_id_type=MESH)
        pl.semaphore_wait(barrier, len(partners))


class Sems:
    def __init__(self, send, recv):
        self.send, self.recv, self.used = send, recv, 0

    def take(self):
        self.used += 1
        return self.send.at[self.used - 1], self.recv.at[self.used - 1]


def remote(src, dst, sems, device):
    return pltpu.make_async_remote_copy(
        src_ref=src, dst_ref=dst, send_sem=sems[0], recv_sem=sems[1], device_id=device, device_id_type=MESH
    )


def rows_at(start, size, unit=16):
    return pl.ds(pl.multiple_of(start, unit), size)


class Gather:
    def __init__(self, where, sems, shard, full, shared, local_sem):
        self.where, self.shard, self.full, self.shared = where, shard, full, shared
        self.rows, self.columns = shard.shape
        self.ring_rows = self.rows - shared
        self.cut = -(-max(self.ring_rows // 2, shared) // 16) * 16
        self.local = pltpu.make_async_copy(
            shard, full.at[rows_at(where.fsdp * self.rows, self.rows)], local_sem
        )
        far = where.far
        take = sems.take
        self.ring_sems = [[take() for _ in range(far)] for _ in range(2)]
        self.across_sems = [[take() for _ in range(far)] for _ in range(2)]
        self.twin_sems = [[take() for _ in range(far)] for _ in range(2)]
        self.twin_across_sems = [[take() for _ in range(far)] for _ in range(2)]
        self.build()

    def columns_of(self, core):
        half = self.columns // 2
        return pl.ds(pl.multiple_of(core * half, 128), half)

    def ring_span(self, direction, step):
        start, size = 0, self.ring_rows
        if step == self.where.far:
            start, size = (0, self.cut) if direction == 0 else (self.cut, self.ring_rows - self.cut)
        return start, size

    def ring_view(self, owner, direction, step, core, ref=None):
        start, size = self.ring_span(direction, step)
        start = start + self.where.plane * self.shared
        if ref is None:
            ref, start = self.full, start + owner * self.rows
        return ref.at[rows_at(start, size), self.columns_of(core)]

    def across_view(self, owner, plane, core):
        start = owner * self.rows + plane * (self.rows - self.shared)
        return self.full.at[rows_at(start, self.shared), self.columns_of(core)]

    def build(self):
        where, far = self.where, self.where.far
        near = range(1, far + 1)
        self.ring_out, self.ring_in, self.across_out, self.across_in = {}, {}, {}, {}
        self.twin_out, self.twin_in, self.twin_across_out, self.twin_across_in = {}, {}, {}, {}
        for direction in range(2):
            to = where.ring[direction]
            src = self.ring_view(None, direction, 1, where.core, self.shard)
            dst = self.ring_view(where.fsdp, direction, 1, where.core)
            self.ring_out[direction, 1] = remote(src, dst, self.ring_sems[direction][0], to)
            for step in near:
                owner = where.owner(direction, step)
                view = self.ring_view(owner, direction, step, where.core)
                self.ring_in[direction, step] = remote(view, view, self.ring_sems[direction][step - 1], to)
                sems = self.twin_sems[direction][step - 1]
                self.twin_out[direction, step] = remote(view, view, sems, where.twin)
                view = self.ring_view(owner, direction, step, 1 - where.core)
                self.twin_in[direction, step] = remote(view, view, sems, where.twin)
                if step < far:
                    view = self.ring_view(owner, direction, step + 1, where.core)
                    self.ring_out[direction, step + 1] = remote(view, view, self.ring_sems[direction][step], to)
                if step < far or direction == 0:
                    sems = self.across_sems[direction][step - 1]
                    view = self.across_view(owner, where.plane, where.core)
                    self.across_out[direction, step] = remote(view, view, sems, where.across)
                    view = self.across_view(owner, 1 - where.plane, where.core)
                    self.across_in[direction, step] = remote(view, view, sems, where.across)
                    sems = self.twin_across_sems[direction][step - 1]
                    self.twin_across_out[direction, step] = remote(view, view, sems, where.twin)
                    view = self.across_view(owner, 1 - where.plane, 1 - where.core)
                    self.twin_across_in[direction, step] = remote(view, view, sems, where.twin)

    def start(self):
        self.local.start()
        for direction in range(2):
            self.ring_out[direction, 1].start()

    def ring_step(self, step):
        far = self.where.far
        for direction in range(2):
            self.ring_in[direction, step].wait_recv()
            if step < far:
                self.ring_out[direction, step + 1].start()
                self.across_out[direction, step].start()
            self.twin_out[direction, step].start()
        if step == far:
            self.across_out[0, step].start()

    def across_step(self, step):
        for direction in range(2 if step < self.where.far else 1):
            self.across_in[direction, step].wait_recv()
            self.twin_across_out[direction, step].start()

    def tick(self, step):
        if step <= self.where.far:
            self.ring_step(step)
        if step > 1:
            self.across_step(step - 1)

    def finish(self):
        for table in (self.twin_in, self.twin_across_in):
            for copy in table.values():
                copy.wait_recv()
        self.local.wait()

    def drain(self):
        for table in (self.ring_out, self.across_out, self.twin_out, self.twin_across_out):
            for copy in table.values():
                copy.wait_send()


class Reduce:
    def __init__(self, where, sems, grad, out, shared, bufs):
        self.where, self.grad, self.out, self.shared = where, grad, out, shared
        self.pair, self.other, self.passing, self.final = bufs
        self.rows = self.pair.shape[0] // where.count
        self.half = self.pair.shape[1]
        self.ring_rows = self.rows - shared
        self.cut = -(-max(self.ring_rows // 2, shared) // 16) * 16
        far, count = where.far, where.count
        order = [(0, far)] + [(d, j) for j in range(far - 1, 0, -1) for d in range(2)] + [(0, 0)]
        self.owners = [self.target(*o) for o in order]
        theirs, mine = self.columns_of(1 - where.core), self.columns_of(where.core)
        self.mine = mine
        self.pair_out, self.other_out, self.other_in, self.ring_out, self.ring_in = [], [], [], {}, {}
        for owner in self.owners:
            rows = rows_at(owner * self.rows, self.rows)
            self.pair_out.append(remote(grad.at[rows, theirs], self.pair.at[rows], sems.take(), where.twin))
            give = rows_at(owner * self.rows + (1 - where.plane) * self.ring_rows, shared)
            came = self.other.at[rows_at(owner * shared, shared)]
            take = sems.take()
            self.other_out.append(remote(self.pair.at[give], came, take, where.across))
            self.other_in.append(remote(came, came, take, where.across))
        for direction in range(2):
            to = where.ring[direction]
            for step in range(1, far + 1):
                start, size = self.span(direction, step)
                rows = self.ring_rows_of(self.target(direction, far + 1 - step), start, size)
                came = self.passing.at[direction, step - 1, pl.ds(start, size)]
                take = sems.take()
                self.ring_out[direction, step] = remote(self.pair.at[rows], came, take, to)
                self.ring_in[direction, step] = remote(came, came, take, to)
        self.own = self.ring_rows_of(where.fsdp, 0, self.ring_rows)
        take = sems.take()
        self.final_out = remote(self.pair.at[self.own], self.final, take, where.across)
        self.final_in = remote(self.final, self.final, take, where.across)
        take = sems.take()
        given, taken = out.at[:, mine], out.at[:, theirs]
        self.out_out = remote(given, given, take, where.twin)
        self.out_in = remote(taken, taken, take, where.twin)

    @staticmethod
    def shapes(rows, columns, count, shared):
        half, ring_rows = columns // 2, rows - shared
        return [
            pltpu.VMEM((count * rows, half), jnp.bfloat16),
            pltpu.VMEM((count * shared, half), jnp.bfloat16),
            pltpu.VMEM((2, count // 2, ring_rows, half), jnp.bfloat16),
            pltpu.VMEM((ring_rows, half), jnp.bfloat16),
        ]

    @staticmethod
    def copies(count):
        return 2 * count + 2 * (count // 2) + 2

    def target(self, direction, distance):
        return self.where.owner(1 - direction, distance)

    def columns_of(self, core):
        return pl.ds(pl.multiple_of(core * self.half, 128), self.half)

    def span(self, direction, step):
        if step > 1:
            return 0, self.ring_rows
        return (0, self.cut) if direction == 0 else (self.cut, self.ring_rows - self.cut)

    def ring_rows_of(self, owner, start, size):
        return rows_at(owner * self.rows + self.where.plane * self.shared + start, size)

    def start(self):
        for copy in self.pair_out:
            copy.start()

    def add_pair(self, start=0, stop=None):
        for i in range(len(self.owners))[start:stop]:
            self.pair_out[i].wait_recv()
            rows = rows_at(self.owners[i] * self.rows, self.rows)
            self.pair[rows, :] = self.pair[rows, :] + self.grad[rows, self.mine]
            self.other_out[i].start()

    def sent_pair(self):
        for copy in self.pair_out:
            copy.wait_send()

    def add_other(self, start=0, stop=None):
        where = self.where
        for i in range(len(self.owners))[start:stop]:
            self.other_in[i].wait_recv()
            owner = self.owners[i]
            mine = rows_at(owner * self.rows + where.plane * self.ring_rows, self.shared)
            theirs = rows_at(owner * self.shared, self.shared)
            self.pair[mine, :] = self.pair[mine, :] + self.other[theirs, :]
            if i == 0:
                self.ring_send(1)

    def go(self, step):
        if step == 0:
            self.add_other(0, 1)
            return
        self.add_other(2 * step - 1, 2 * step + 1)
        self.ring_step(step)

    def ring_send(self, step):
        for direction in range(2):
            self.ring_out[direction, step].start()

    def ring_step(self, step):
        far = self.where.far
        for direction in range(2):
            start, size = self.span(direction, step)
            self.ring_in[direction, step].wait_recv()
            if step < far:
                rows = self.ring_rows_of(self.target(direction, far - step), start, size)
                came = self.passing[direction, step - 1, pl.ds(start, size)]
                self.pair[rows, :] = self.pair[rows, :] + came
        if step < far:
            self.ring_send(step + 1)
            return
        total = self.pair[self.own, :].astype(jnp.float32)
        total = total + self.passing[0, step - 1].astype(jnp.float32)
        total = total + self.passing[1, step - 1].astype(jnp.float32)
        self.pair[self.own, :] = total.astype(jnp.bfloat16)
        self.final_out.start()

    def finish(self):
        where = self.where
        self.final_in.wait_recv()
        columns = self.mine
        plane, shared, ring_rows = where.plane, self.shared, self.ring_rows
        both = self.rows - 2 * shared
        base = where.fsdp * self.rows + plane * shared
        f32 = jnp.float32
        if both:
            mine = self.pair[rows_at(base + (1 - plane) * shared, both), :].astype(f32)
            theirs = self.final[rows_at(plane * shared, both), :].astype(f32)
            self.out[pl.ds(shared, both), columns] = mine + theirs
        mine = self.pair[rows_at(base + plane * (ring_rows - shared), shared), :]
        self.out[rows_at(plane * ring_rows, shared), columns] = mine.astype(f32)
        theirs = self.final[rows_at((1 - plane) * (ring_rows - shared), shared), :]
        self.out[rows_at((1 - plane) * ring_rows, shared), columns] = theirs.astype(f32)
        self.out_out.start()

    def close(self):
        self.out_in.wait_recv()
        for copy in self.other_out + list(self.ring_out.values()) + [self.final_out, self.out_out]:
            copy.wait_send()


FORWARD_ORDER = {
    "entry": ((1, 0), (0, 0),),
    "bias": ((2, 0), (1, 1), (0, 1), (2, 1),),
    "norm": ((1, 2), (0, 2), (3, 0), (1, 3), (2, 2), (0, 3), (4, 0), (3, 1), (1, 4), (5, 0), (0, 4), (6, 0),),
    "tables": ((1, 5), (0, 5), (1, 6), (2, 3), (3, 2), (0, 6),),
    "q": ((5, 1), (4, 1),),
    "k": ((2, 4), (6, 1),),
    "v": ((3, 3),),
    "pair1": ((5, 2),),
    "pair2": ((2, 5),),
    "pair3": ((2, 6), (4, 2), (3, 4),),
    "pair4": ((6, 2),),
    "pair5": ((4, 3), (5, 3),),
    "mix": ((3, 5),),
    "norm2": ((3, 6), (4, 4), (6, 3),),
    "hid1": ((4, 5), (5, 4), (6, 4), (4, 6),),
    "hid2": ((5, 5),),
    "hid3": ((5, 6),),
    "res0": ((6, 5),),
    "res1": ((6, 6),),
}
BACKWARD_ORDER = {
    "hid1": ((8, -1),),
    "hid3": ((8, -2),),
    "dw1_2": ((8, 0),),
    "dw1_3": ((0, -1), (1, -1), (2, -1),),
    "ng1": ((8, 1), (0, 0),),
    "nb2": ((1, 0), (3, -1),),
    "mixb": ((0, 1), (8, 2), (2, 0),),
    "bias": ((3, 0), (1, 1), (4, -1),),
    "pair0": ((4, 0),),
    "pair1": ((8, 3), (3, 1), (0, 2),),
    "pair3": ((4, 1), (2, 1), (5, -1), (3, 2), (1, 2),),
    "pair4": ((5, 0), (8, 4), (6, -1), (2, 2), (4, 2), (0, 3),),
    "pair5": ((5, 1),),
    "ox0": ((1, 3), (6, 0), (7, -1), (4, 3),),
    "ox1": ((3, 3),),
    "ox2": ((7, 0), (6, 1), (2, 3),),
    "nb1": ((7, 1), (1, 4), (0, 4), (6, 2),),
    "pack": ((5, 2), (9, 0), (3, 4), (7, 2), (2, 4), (9, 1), (6, 3), (1, 5), (4, 4), (5, 3), (0, 5), (7, 3), (8, 5), (2, 5), (6, 4), (9, 2), (3, 5), (5, 4), (4, 5), (7, 4), (6, 5), (9, 3), (5, 5), (7, 5),),
}


SEG_ROWS = (1, 1, 3, 2, 1, 1, 1, 4, 1)
(G1, B1, QB, FR, OB, G2, B2, F1B, F2B) = range(9)
MLP = 3072


def offsets():
    starts, total = [], 0
    for m in SEG_ROWS:
        starts.append(total)
        total += m
    return starts, total


def unpack_small(slots, vec, count, seg):
    lane = lax.broadcasted_iota(jnp.int32, (1, 128), 1)
    starts, _ = offsets()
    for first, m in zip(starts, SEG_ROWS):
        pieces = [jnp.zeros((1, 128), jnp.float32) for _ in range(m * count * seg // 128)]
        for f in range(count):
            for i in range(m):
                at = (m * f + i) * seg
                v, s = at // 128, at % 128
                row = slots[f, first + i : first + i + 1, :]
                if s:
                    row = pltpu.roll(row, s, 1)
                pieces[v] = pieces[v] + jnp.where(lane >= s, row, 0.0)
                if s + seg > 128:
                    pieces[v + 1] = pieces[v + 1] + jnp.where(lane < s + seg - 128, row, 0.0)
        for v, piece in enumerate(pieces):
            at = first * count * seg + 128 * v
            vec[:, at : at + 128] = piece


def part_of(vec, which, start=0, size=None):
    starts, _ = offsets()
    base = starts[which] * D
    size = SEG_ROWS[which] * D if size is None else size
    return vec[:, base + start : base + start + size]


def half_swap(t):
    width = t.shape[-1]
    lane = lax.broadcasted_iota(jnp.int32, t.shape, 1)
    return jnp.where(lax.rem(lane, HD) < HD // 2, pltpu.roll(t, width - HD // 2, 1), pltpu.roll(t, HD // 2, 1))


def columns_down(ref, i):
    return jnp.broadcast_to(ref[i : i + 1, :], (128, 128)).T


def rope_tables(vec, col, row, cosine, sine, tables):
    step = lax.broadcasted_iota(jnp.int32, (32, D), 0).astype(jnp.float32)
    stacks = []
    for at in (0, D):
        angle = step * part_of(vec, FR, at, D)
        for table in (jnp.cos(angle), jnp.sin(angle)):
            high = table.astype(jnp.bfloat16)
            rest = table - high.astype(jnp.float32)
            middle = rest.astype(jnp.bfloat16)
            last = (rest - middle.astype(jnp.float32)).astype(jnp.bfloat16)
            stacks.append(jnp.concatenate([high, middle, last, jnp.zeros_like(high)], axis=0))
            tables[len(stacks) - 1] = stacks[-1]
    lane = lax.broadcasted_iota(jnp.int32, (128, 128), 1)
    slot = jnp.where(lane < 96, lax.rem(lane, 32), -1).astype(jnp.float32)
    wide = lax.broadcasted_iota(jnp.int32, (128, D), 1)
    sign = jnp.where(lax.rem(wide, HD) < HD // 2, -1.0, 1.0)
    for i in range(col.shape[0]):
        at = pl.ds(128 * i, 128)
        pick_col = jnp.where(columns_down(col, i) == slot, 1.0, 0.0).astype(jnp.bfloat16)
        pick_row = jnp.where(columns_down(row, i) == slot, 1.0, 0.0).astype(jnp.bfloat16)
        look = lambda pick, stack: jnp.dot(pick, stack, preferred_element_type=jnp.float32)
        cc, cs = look(pick_col, stacks[0]), look(pick_col, stacks[1])
        rc, rs = look(pick_row, stacks[2]), look(pick_row, stacks[3])
        cosine[at, :] = cc * rc - cs * rs
        sine[at, :] = (cs * rc + cc * rs) * sign


def image_bias(image, bias):
    for i in range(image.shape[0]):
        mine = columns_down(image, i)
        for j in range(image.shape[0]):
            same = mine == image[j : j + 1, :]
            bias[128 * i : 128 * i + 128, 128 * j : 128 * j + 128] = jnp.where(same, 0.0, MASKED)


def turn(source, target, start=0):
    def body(j):
        target[pl.ds(pl.multiple_of(start + 128 * j, 128), 128), :] = source[:, tile_at(j, 128)].T

    loop(source.shape[1] // 128, body)


def statistics(values):
    centre = values - jnp.mean(values, axis=-1, keepdims=True)
    spread = jnp.mean(centre * centre, axis=-1, keepdims=True)
    inverse = lax.rsqrt(spread + EPSILON)
    return centre * inverse, inverse


def loop(count, body):
    def run(i, carry):
        body(i)
        return carry

    lax.fori_loop(0, count, run, 0)


def tile_at(i, size):
    return pl.ds(pl.multiple_of(i * size, size), size)


def matmul(left, right):
    return jnp.dot(left, right, preferred_element_type=jnp.float32)


def matmul_nt(left, right):
    return lax.dot_general(left, right, (((1,), (1,)), ((), ())), preferred_element_type=jnp.float32)


def project(normed_low, weights, vec, cosine, sine, outs, at):
    tile = 256
    per = D // tile
    for which, out in enumerate(outs):
        def body(j, which=which, out=out):
            cols = tile_at(j, tile)
            wide = pl.ds(pl.multiple_of(which * D + j * tile, tile), tile)
            starts, _ = offsets()
            shift = vec[:, pl.ds(pl.multiple_of(starts[QB] * D + which * D + j * tile, tile), tile)]
            t = matmul(normed_low[...], weights[:, wide]) + shift
            if which < 2:
                t = t * cosine[:, cols] + half_swap(t) * sine[:, cols]
            if which == 0:
                t = t * HD**-0.5
            out[:, cols] = t.astype(jnp.bfloat16)

        loop(per, body)
        at("qkv"[which])


def attend(pair, query, key, value, bias, mixed, lse, block):
    lane_all = lax.broadcasted_iota(jnp.int32, (1, 128), 1)
    cols = tile_at(pair, 128)
    lane = lax.broadcasted_iota(jnp.int32, (1, 128), 1)
    first = lane < HD
    k2, v2 = key[:, cols], value[:, cols]
    zero = jnp.zeros((), jnp.bfloat16)
    for start in range(0, query.shape[0], block):
        rows = pl.ds(start, block)
        q2 = query[rows, cols]
        total, sums, tops = None, [], []
        for keep in (first, ~first):
            s = matmul_nt(jnp.where(keep, q2, zero), k2) + bias[rows, :]
            top = jnp.max(s, axis=-1, keepdims=True)
            p = jnp.exp(s - top)
            sums.append(jnp.sum(p, axis=-1, keepdims=True))
            tops.append(top)
            o = matmul(p.astype(jnp.bfloat16), jnp.where(keep, v2, zero))
            total = o if total is None else total + o
        mixed[rows, cols] = (total / jnp.where(first, sums[0], sums[1])).astype(jnp.bfloat16)
        kept = lse[rows, :]
        for i in range(2):
            kept = jnp.where(lane_all == 2 * pair + i, tops[i] + jnp.log(sums[i]), kept)
        lse[rows, :] = kept


def norm_rows(source, normed_low, vec, gain, shift, block=128):
    def body(i):
        rows = tile_at(i, block)
        unit, _ = statistics(source[rows, :].astype(jnp.float32))
        normed_low[rows, :] = (unit * part_of(vec, gain) + part_of(vec, shift)).astype(jnp.bfloat16)

    loop(source.shape[0] // block, body)


def mix_out(x, mixed, weights, vec, middle):
    starts, _ = offsets()

    def body(j):
        cols = tile_at(j, 256)
        shift = vec[:, pl.ds(pl.multiple_of(starts[OB] * D + j * 256, 256), 256)]
        middle[:, cols] = x[:, cols].astype(jnp.float32) + matmul(mixed[...], weights[:, cols]) + shift

    loop(D // 256, body)


def hidden_tile(j, normed_low, weights, vec, active, active_t, slope):
    starts, _ = offsets()
    cols = tile_at(j, 256)
    shift = vec[:, pl.ds(pl.multiple_of(starts[F1B] * D + j * 256, 256), 256)]
    h = matmul(normed_low[...], weights[:, cols]) + shift
    c = (2.0 / math.pi) ** 0.5
    square = h * h
    t = jnp.tanh(c * h * (1.0 + 0.044715 * square))
    low = (0.5 * h * (1.0 + t)).astype(jnp.bfloat16)
    active[:, cols] = low
    active_t[cols, :] = low.T
    slope[:, cols] = (
        0.5 * (1.0 + t) + 0.5 * h * (1.0 - t * t) * (c * (1.0 + 3 * 0.044715 * square))
    ).astype(jnp.bfloat16)


def result_tile(j, middle, active, weights, vec, output):
    starts, _ = offsets()
    cols = tile_at(j, 256)
    shift = vec[:, pl.ds(pl.multiple_of(starts[F2B] * D + j * 256, 256), 256)]
    output[:, cols] = (middle[:, cols] + matmul(active[...], weights[:, cols]) + shift).astype(jnp.bfloat16)


def forward_kernel(count, seg, *refs):
    (x, image, row, col, small, qkv_s, out_s, fc1_s, fc2_s) = refs[:9]
    (output, vec_o, tables_o, turned_o, q_o, k_o, v_o, lse_o, middle_o, act_t_o, slope_o,
     qkv_o, out_o, fc1_o, fc2_o) = refs[9:24]
    (slots, vec, tables, turned, q, k, v, lse_t, middle, act_t, slope, qkv_w, out_w, fc1_w, fc2_w,
     cosine, sine, bias, lse, act, low,
     send, recv, small_send, small_recv, local, saved) = refs[24:]
    n1 = mixed = n2 = low
    where = Place(count)
    peers = [(lax.rem(where.fsdp + i, count), where.dp) for i in range(1, count)]
    where.greet(peers)
    sems = Sems(send, recv)
    cuts = (
        (qkv_s, qkv_w, 0, 1280), (qkv_s, qkv_w, 1280, 1024), (out_s, out_w, 0, D),
        (fc1_s, fc1_w, 0, MLP // 2), (fc1_s, fc1_w, MLP // 2, MLP // 2), (fc2_s, fc2_w, 0, 512), (fc2_s, fc2_w, 512, 256),
    )
    flows = [
        Gather(where, sems, s.at[:, pl.ds(at, size)], w.at[:, pl.ds(at, size)], s.shape[0] // 3, local.at[i])
        for i, (s, w, at, size) in enumerate(cuts)
    ]

    def at(point):
        for i, step in FORWARD_ORDER.get(point, ()):
            if step == 0:
                flows[i].start()
            elif step <= where.far + 1:
                flows[i].tick(step)
            else:
                flows[i].finish()

    small_copies = [
        remote(small, slots.at[where.fsdp], (small_send.at[i], small_recv.at[i]), peers[i])
        for i in range(count - 1)
    ]
    for copy in small_copies:
        copy.start()
    at("entry")
    slots[where.fsdp] = small[...]
    saves = []

    def save(source, target):
        copy = pltpu.make_async_copy(source, target, saved.at[len(saves)])
        copy.start()
        saves.append(copy)

    image_bias(image, bias)
    for i in range(1, count):
        came = slots.at[lax.rem(where.fsdp + count - i, count)]
        remote(came, came, (small_send.at[i - 1], small_recv.at[i - 1]), peers[i - 1]).wait_recv()
    unpack_small(slots, vec, count, seg)
    save(vec, vec_o)
    at("bias")
    norm_rows(x, n1, vec, G1, B1)
    turn(n1, turned)
    lse[...] = jnp.zeros_like(lse)
    at("norm")
    rope_tables(vec, col, row, cosine, sine, tables)
    save(tables, tables_o)
    at("tables")
    project(n1, qkv_w, vec, cosine, sine, (q, k, v), at)
    save(qkv_w, qkv_o)
    save(q, q_o)
    save(k, k_o)
    save(v, v_o)

    def pair_body(j):
        attend(j, q, k, v, bias, mixed, lse, 320)
        for i in range(H // 2):
            @pl.when(j == i)
            def _(i=i):
                at(f"pair{i}")

    loop(H // 2, pair_body)
    lse_t[...] = lse[...].T
    save(lse_t, lse_o)
    turn(mixed, turned, D)
    save(out_w, out_o)
    mix_out(x, mixed, out_w, vec, middle)
    save(middle, middle_o)
    at("mix")
    norm_rows(middle, n2, vec, G2, B2)
    turn(n2, turned, 2 * D)
    save(turned, turned_o)
    at("norm2")
    for i in range(4):
        loop(MLP // 1024, lambda j: hidden_tile(MLP // 1024 * i + j, n2, fc1_w, vec, act, act_t, slope))
        at(f"hid{i}")
    save(act_t, act_t_o)
    save(slope, slope_o)
    save(fc1_w, fc1_o)
    for i in range(D // 256):
        result_tile(i, middle, act, fc2_w, vec, output)
        at(f"res{i}")
    save(fc2_w, fc2_o)
    for flow in flows:
        flow.drain()
    for copy in small_copies:
        copy.wait_send()
    for copy in saves:
        copy.wait()


def forward(x, image, row, col, small, weights, count):
    bf16, f32 = jnp.bfloat16, jnp.float32
    tokens = x.shape[0]
    seg = D // count
    wide = lambda kind, width=D: ((tokens, width), kind)
    total = offsets()[1] * D
    full = [((w.shape[0] * count, w.shape[1]), bf16) for w in weights]
    kept = [
        ((1, total), f32), ((4, 128, D), bf16), ((3 * D, tokens), bf16), wide(bf16), wide(bf16), wide(bf16),
        ((128, tokens), f32), wide(f32), ((MLP, tokens), bf16), wide(bf16, MLP),
    ] + full
    copies = 7 * 8 * (count // 2)
    any_spec = pl.BlockSpec(memory_space=pl.ANY)
    vmem_spec = pl.BlockSpec(memory_space=pltpu.VMEM)
    scratch = kept + [
        wide(f32), wide(f32), ((tokens, tokens), f32), wide(f32, 128), wide(bf16, MLP), wide(bf16),
    ]
    return pl.pallas_call(
        partial(forward_kernel, count, seg),
        out_shape=[jax.ShapeDtypeStruct((tokens, D), bf16)] + [jax.ShapeDtypeStruct(*s) for s in kept],
        in_specs=[vmem_spec] * 9,
        out_specs=[vmem_spec] + [any_spec] * len(kept),
        scratch_shapes=[pltpu.VMEM((count,) + small.shape, f32)]
        + [pltpu.VMEM(*s) for s in scratch]
        + [
            pltpu.SemaphoreType.DMA((copies,)),
            pltpu.SemaphoreType.DMA((copies,)),
            pltpu.SemaphoreType.DMA((count - 1,)),
            pltpu.SemaphoreType.DMA((count - 1,)),
            pltpu.SemaphoreType.DMA((7,)),
            pltpu.SemaphoreType.DMA((len(kept),)),
        ],
        compiler_params=pltpu.CompilerParams(
            collective_id=0, has_side_effects=True, vmem_limit_bytes=67043328
        ),
        name="forward",
    )(x, image, row, col, small, *weights)


def unit_and_inverse(source, rows):
    return statistics(source[rows, :].astype(jnp.float32))


def attend_back(pair, query, key, value, lse_t, bias, tables, pick_col, pick_row, colb, rowb, given, grads, sums, blocks):
    cols = tile_at(pair, 128)
    f32, bf16 = jnp.float32, jnp.bfloat16
    tokens = query.shape[0]
    lane = lax.broadcasted_iota(jnp.int32, (1, 128), 1)
    first = lane < HD
    zero = jnp.zeros((), bf16)
    q2, k2, v2, g2 = query[:, cols], key[:, cols], value[:, cols], given[:, cols]
    k2_t = k2.T
    grad_key = jnp.zeros((tokens, 128), f32)
    grad_value = jnp.zeros((tokens, 128), f32)
    turned = []
    for start, size in blocks:
        rows = slice(start, start + size)
        halves = []
        for i, keep in enumerate((first, ~first)):
            q1 = jnp.where(keep, q2[rows], zero)
            g1 = jnp.where(keep, g2[rows], zero)
            s = matmul_nt(k2, q1) + bias[:, rows]
            heads = lse_t[0:16, rows]
            head = lax.broadcasted_iota(jnp.int32, heads.shape, 0)
            p = jnp.exp(s - jnp.sum(jnp.where(head == 2 * pair + i, heads, 0.0), axis=0, keepdims=True))
            gp = matmul_nt(v2, g1)
            ds = p * (gp - jnp.sum(p * gp, axis=0, keepdims=True))
            ds = ds.astype(bf16)
            grad_value = grad_value + matmul(p.astype(bf16), g1)
            grad_key = grad_key + matmul(ds, q1)
            halves.append(matmul(k2_t[HD * i : HD * i + HD], ds))
        turned.append(jnp.concatenate(halves, axis=0).T)
    grad_query = jnp.concatenate(turned, axis=0) * HD**-0.5
    look = lambda pick, i: jnp.dot(pick[...], tables[i, :, cols], preferred_element_type=f32)
    cc, cs, rc, rs = look(pick_col, 0), look(pick_col, 1), look(pick_row, 2), look(pick_row, 3)
    sign = jnp.where(lax.rem(lane, HD) < HD // 2, -1.0, 1.0)
    cosine, sine = cc * rc - cs * rs, (cs * rc + cc * rs) * sign
    turn_sum = half_swap(q2.astype(f32)) * (grad_query * HD**0.5) + half_swap(k2.astype(f32)) * grad_key
    starts, _ = offsets()
    for i, where_at in enumerate((colb, rowb)):
        at = pl.ds(pl.multiple_of((starts[FR] + i) * D + 128 * pair, 128), 128)
        sums[:, at] = jnp.sum(turn_sum * where_at[...], axis=0, keepdims=True) * sign
    finals = (
        grad_query * cosine - half_swap(grad_query) * sine,
        grad_key * cosine - half_swap(grad_key) * sine,
        grad_value,
    )
    for i, final in enumerate(finals):
        low = final.astype(bf16)
        at = pl.ds(pl.multiple_of(i * D + 128 * pair, 128), 128)
        grads[:, at] = low
        at = pl.ds(pl.multiple_of((starts[QB] + i) * D + 128 * pair, 128), 128)
        sums[:, at] = jnp.sum(low.astype(f32), axis=0, keepdims=True)


def norm_back(source, grad, onward, gain, vec, sums, which_gain, which_shift, emit, block=128):
    starts, _ = offsets()
    gain_at = slice(starts[which_gain] * D, starts[which_gain] * D + D)
    shift_at = slice(starts[which_shift] * D, starts[which_shift] * D + D)
    sums[:, gain_at] = jnp.zeros((1, D), jnp.float32)
    sums[:, shift_at] = jnp.zeros((1, D), jnp.float32)

    def body(i):
        rows = tile_at(i, block)
        unit, inverse = statistics(source[rows, :].astype(jnp.float32))
        g = grad[rows, :]
        sums[:, gain_at] += jnp.sum(g * unit, axis=0, keepdims=True)
        sums[:, shift_at] += jnp.sum(g, axis=0, keepdims=True)
        e = g * part_of(vec, gain)
        mean = jnp.mean(e, axis=-1, keepdims=True)
        along = jnp.mean(e * unit, axis=-1, keepdims=True)
        emit(rows, onward[rows, :].astype(jnp.float32) + inverse * (e - mean - unit * along))

    loop(source.shape[0] // block, body)


def pack_sums(sums, slots, count, seg):
    lane = lax.broadcasted_iota(jnp.int32, (1, 128), 1)
    starts, _ = offsets()
    slots[...] = jnp.zeros_like(slots)
    for first, m in zip(starts, SEG_ROWS):
        for f in range(count):
            for i in range(m):
                at = first * count * seg + (m * f + i) * seg
                v, s = at // 128, at % 128
                row = sums[:, 128 * v : 128 * v + 128]
                if s:
                    row = pltpu.roll(row, 128 - s, 1)
                if s + seg > 128:
                    more = pltpu.roll(sums[:, 128 * v + 128 : 128 * v + 256], 128 - s, 1)
                    row = jnp.where(lane < 128 - s, row, more)
                slots[f, first + i : first + i + 1, :] = jnp.where(lane < seg, row, 0.0)


def backward_kernel(count, seg, shares, wide_shared, *refs):
    (x, grad_out, image, row, col, vec_h, tables_h, turned_h, q_h, k_h, v_h, lse_h, middle_h, act_t_h, slope_h,
     qkv_h, out_h, fc1_h, fc2_h) = refs[:19]
    (grad_x, small_out, grad_qkv, grad_out_w, grad_fc1, grad_fc2) = refs[19:25]
    (vec, tables, q, k, v, lse_t, middle, act_t, slope, out_w, fc1_w, fc2_w,
     bias, pick_col, pick_row, colb, rowb, wide, low, big, sums, slots, slots_twin, slots_across, slots_in) = refs[25:50]
    outs = refs[50:57]
    bufs = refs[57:93]
    send, recv, small_send, small_recv, loaded = refs[93:]
    f32, bf16 = jnp.float32, jnp.bfloat16
    where = Place(count)
    far = where.far
    starts, _ = offsets()

    loads = {}

    def load(name, source, target):
        copy = pltpu.make_async_copy(source, target, loaded.at[len(loads)])
        copy.start()
        loads[name] = copy

    load("act", act_t_h, act_t)
    peers = [(lax.rem(where.fsdp + i, count), where.dp) for i in range(1, count)]
    where.greet(peers)
    sems = Sems(send, recv)
    fc2 = Reduce(where, sems, big, grad_fc2, wide_shared, bufs[:4])
    parts = [
        Reduce(
            where, sems, big.at[pl.ds(D * (i % 4), D)], grad_out_w if i == 4 else outs[i - (i > 4)],
            shares[i], bufs[4 + 4 * i : 8 + 4 * i],
        )
        for i in range(8)
    ]

    loads["act"].wait()
    load("fc2", fc2_h, fc2_w)
    load("slope", slope_h, slope)
    loop(8, lambda i: store_tile(big, i, 384, act_t, grad_out))
    fc2.start()
    at = starts[F2B] * D
    sums[:, at : at + D] = jnp.sum(grad_out[...].astype(f32), axis=0, keepdims=True)
    loads["fc2"].wait()
    loads["slope"].wait()
    load("turned", turned_h, act_t.at[pl.ds(0, 3 * D)])
    load("fc1", fc1_h, fc1_w)
    for name, source, target in (
        ("vec", vec_h, vec), ("middle", middle_h, middle), ("out", out_h, out_w), ("q", q_h, q), ("k", k_h, k),
        ("v", v_h, v), ("lse", lse_h, lse_t), ("tables", tables_h, tables),
    ):
        load(name, source, target)
    normed_one, mixed_t, normed_two = (act_t.at[pl.ds(D * i, D)] for i in range(3))

    def hidden(j):
        cols = tile_at(j, 256)
        g = matmul_nt(grad_out[...], fc2_w[cols, :]) * slope[:, cols].astype(f32)
        g = g.astype(bf16)
        slope[:, cols] = g
        at = pl.ds(pl.multiple_of(starts[F1B] * D + 256 * j, 256), 256)
        sums[:, at] = jnp.sum(g.astype(f32), axis=0, keepdims=True)

    take = lambda i: (small_send.at[i], small_recv.at[i])
    to_twin = remote(slots, slots_twin, take(0), where.twin)
    to_across = remote(slots, slots_across, take(1), where.across)
    given = [
        remote(slots.at[peer[0]], slots_in.at[where.fsdp], take(2 + i), peer) for i, peer in enumerate(peers)
    ]
    every = parts + [fc2]

    def small_step(step):
        if step == 0:
            to_twin.start()
        elif step == 1:
            to_twin.wait()
            slots[...] = slots[...] + slots_twin[...]
            to_across.start()
        elif step == 2:
            to_across.wait()
            slots[...] = slots[...] + slots_across[...]
            slots_in[where.fsdp] = slots[where.fsdp]
            for copy in given:
                copy.start()
        else:
            for i in range(1, count):
                came = slots_in.at[lax.rem(where.fsdp + count - i, count)]
                remote(came, came, take(1 + i), peers[i - 1]).wait_recv()
            total = slots_in[0]
            for i in range(1, count):
                total = total + slots_in[i]
            small_out[...] = total

    def reach(point):
        for i, step in BACKWARD_ORDER.get(point, ()):
            if i == 9:
                small_step(step)
            elif step < 0:
                bounds = ((0, None),) if i < 8 else ((0, 3), (3, None))
                every[i].add_pair(*bounds[-1 - step])
            elif step <= far:
                every[i].go(step)
            else:
                every[i].finish()

    reach("dw2")
    for i in range(4):
        loop(MLP // 1024, lambda j: hidden(MLP // 1024 * i + j))
        reach(f"hid{i}")
    fc2.sent_pair()
    loads["turned"].wait()
    for i in range(4):
        grad_part = slope.at[:, pl.ds(D * i, D)]
        loop(2, lambda j: store_tile(big.at[pl.ds(D * i, D)], j, 384, normed_two, grad_part))
        parts[i].start()
        reach(f"dw1_{i}")
    loads["fc1"].wait()

    def normed_grad(j):
        cols = tile_at(j, 256)
        wide[:, cols] = matmul_nt(slope[...], fc1_w[cols, :])

    for i in range(3):
        normed_grad(i)
        reach(f"ng{i}")
    for i in range(4):
        parts[i].sent_pair()
    load("qkv", qkv_h, big_rows(fc1_w))
    loads["vec"].wait()
    loads["middle"].wait()

    at = starts[OB] * D
    sums[:, at : at + D] = jnp.zeros((1, D), f32)

    def keep_middle(rows, total):
        wide[rows, :] = total
        total = total.astype(bf16)
        low[rows, :] = total
        sums[:, at : at + D] += jnp.sum(total.astype(f32), axis=0, keepdims=True)

    norm_back(middle, wide, grad_out, G2, vec, sums, G2, B2, keep_middle)
    reach("nb2")
    loop(2, lambda j: store_tile(big.at[pl.ds(0, D)], j, 384, mixed_t, low))
    parts[4].start()
    reach("dwo")
    loads["out"].wait()
    mixed_grad = slope.at[:, pl.ds(3 * D, D)]

    def mix_back(j):
        cols = tile_at(j, 256)
        mixed_grad[:, cols] = matmul_nt(low[...], out_w[cols, :]).astype(bf16)

    loop(D // 256, mix_back)
    reach("mixb")

    image_bias(image, bias)
    lane = lax.broadcasted_iota(jnp.int32, (128, 128), 1)
    slot = jnp.where(lane < 96, lax.rem(lane, 32), -1).astype(f32)
    for i in range(col.shape[0]):
        rows = slice(128 * i, 128 * i + 128)
        for source, kept, pick in ((col, colb, pick_col), (row, rowb, pick_row)):
            down = columns_down(source, i)
            kept[rows, :] = down
            pick[rows, :] = jnp.where(down == slot, 1.0, 0.0).astype(bf16)
    for name in ("q", "k", "v", "lse", "tables"):
        loads[name].wait()

    reach("bias")
    tokens = q.shape[0]
    blocks = [(i, min(256, tokens - i)) for i in range(0, tokens, 256)]

    def pair_body(j):
        attend_back(
            j, q, k, v, lse_t, bias, tables, pick_col, pick_row, colb, rowb, mixed_grad, slope, sums, blocks
        )
        for i in range(H // 2):
            @pl.when(j == i)
            def _(i=i):
                if i % 2:
                    project_back(parts[5 + i // 2].grad, normed_one, slope, i // 2)
                    parts[5 + i // 2].start()
                reach(f"pair{i}")

    loop(H // 2, pair_body)
    loads["qkv"].wait()
    qkv_w = big_rows(fc1_w)
    def normed_one_grad(j):
        cols = tile_at(j, 256)
        middle[:, cols] = matmul_nt(slope[:, pl.ds(0, 3 * D)], qkv_w[cols, :])

    for i in range(3):
        normed_one_grad(i)
        reach(f"ox{i}")

    def keep_x(rows, total):
        grad_x[rows, :] = total.astype(bf16)

    norm_back(x, middle, wide, G1, vec, sums, G1, B1, keep_x)
    reach("nb1")
    pack_sums(sums, slots, count, seg)
    reach("pack")
    for copy in given:
        copy.wait_send()
    for i in range(4, 8):
        parts[i].sent_pair()
    fc2.close()
    for part in parts:
        part.close()
    for i in range(4):
        grad_fc1[:, pl.ds(D * i, D)] = outs[i][...]
    for m in range(3):
        for i in range(3):
            grad_qkv[:, pl.ds(i * D + 256 * m, 256)] = outs[4 + m][:, pl.ds(256 * i, 256)]


def store_tile(target, i, size, left, right):
    rows = tile_at(i, size)
    target[rows, :] = matmul(left[rows, :], right[...]).astype(jnp.bfloat16)


def big_rows(ref):
    return ref.at[:, pl.ds(0, 3 * D)]


def project_back(target, normed, grads, m):
    for i in range(3):
        target[:, pl.ds(256 * i, 256)] = matmul(normed[...], grads[:, pl.ds(i * D + 256 * m, 256)]).astype(jnp.bfloat16)


def backward(x, grad_out, image, row, col, kept, count):
    bf16, f32 = jnp.bfloat16, jnp.float32
    tokens = x.shape[0]
    seg = D // count
    shares, wide_shared = tuple(16 + 16 * (i % 2) for i in range(8)), seg
    (vec, tables, turned, q, k, v, lse, middle, act_t, slope, qkv, out, fc1, fc2) = kept
    like = lambda a: pltpu.VMEM(a.shape, a.dtype)
    side = pltpu.VMEM((tokens, 128), f32)
    pick = pltpu.VMEM((tokens, 128), bf16)
    slots = pltpu.VMEM((count, 16, 128), f32)
    part = pltpu.VMEM((seg, D), f32)
    flows = Reduce.shapes(MLP // count, D, count, wide_shared)
    for shared in shares:
        flows = flows + Reduce.shapes(seg, D, count, shared)
    copies = 9 * Reduce.copies(count)
    any_spec = pl.BlockSpec(memory_space=pl.ANY)
    vmem_spec = pl.BlockSpec(memory_space=pltpu.VMEM)
    dma = pltpu.SemaphoreType.DMA
    return pl.pallas_call(
        partial(backward_kernel, count, seg, shares, wide_shared),
        out_shape=[
            jax.ShapeDtypeStruct((tokens, D), bf16),
            jax.ShapeDtypeStruct((16, 128), f32),
            jax.ShapeDtypeStruct((seg, 3 * D), f32),
            jax.ShapeDtypeStruct((seg, D), f32),
            jax.ShapeDtypeStruct((seg, MLP), f32),
            jax.ShapeDtypeStruct((MLP // count, D), f32),
        ],
        in_specs=[vmem_spec] * 5 + [any_spec] * len(kept),
        out_specs=[vmem_spec] * 6,
        scratch_shapes=[like(a) for a in (vec, tables, q, k, v, lse, middle, act_t, slope, out, fc1, fc2)]
        + [
            pltpu.VMEM((tokens, tokens), f32), pick, pick, side, side,
            pltpu.VMEM((tokens, D), f32), pltpu.VMEM((tokens, D), bf16), pltpu.VMEM((MLP, D), bf16),
            pltpu.VMEM(vec.shape, f32), slots, slots, slots, slots,
        ]
        + [part] * 7
        + flows
        + [dma((copies,)), dma((copies,)), dma((count + 1,)), dma((count + 1,)), dma((len(kept),))],
        compiler_params=pltpu.CompilerParams(
            collective_id=1, has_side_effects=True, vmem_limit_bytes=67043328
        ),
        name="backward",
    )(x, grad_out, image, row, col, *kept)


def pack_small(parts, count):
    seg = D // count
    rows = []
    for i, part in enumerate(parts):
        if i == FR:
            part = jnp.broadcast_to(part.reshape(-1, 1, HD // 2), (seg // (HD // 2), 2, HD // 2))
        rows.append(part.reshape(-1, seg))
    rows = jnp.concatenate(rows, axis=0).astype(jnp.float32)
    return jnp.pad(rows, ((0, -rows.shape[0] % 8), (0, 128 - seg)))


def normed(values, scales, shifts):
    centre = values - jnp.mean(values, axis=-1, keepdims=True)
    spread = jnp.mean(centre * centre, axis=-1, keepdims=True)
    return centre * lax.rsqrt(spread + EPSILON) * scales + shifts


def rotate(queries, keys_in, frequency, row_pos, col_pos):
    half_dim = queries.shape[-1] // 2
    head_count = queries.shape[1]
    split_at = head_count * half_dim
    along_col = frequency[:split_at].reshape(head_count, half_dim)
    along_row = frequency[split_at:].reshape(head_count, half_dim)
    angles = col_pos[:, None, None] * along_col[None] + row_pos[:, None, None] * along_row[None]
    cosine = jnp.cos(angles)
    sine_part = jnp.sin(angles)

    def turned(operand):
        first_half = operand[..., :half_dim]
        second_half = operand[..., half_dim:]
        return jnp.concatenate(
            [
                first_half * cosine - second_half * sine_part,
                first_half * sine_part + second_half * cosine,
            ],
            axis=-1,
        )

    return (turned(queries), turned(keys_in))


def body(
    layer_in,
    ln1_gain,
    ln1_bias,
    qkv_weight,
    qkv_bias,
    rope_freqs,
    out_weight,
    out_bias,
    ln2_gain,
    ln2_bias,
    fc1_weight,
    fc1_bias,
    fc2_weight,
    fc2_bias,
    image_of,
    patch_row,
    patch_col,
    grad_out,
):
    gathered = (
        lax.all_gather(ln1_gain, "fsdp", axis=0, tiled=True),
        lax.all_gather(ln1_bias, "fsdp", axis=0, tiled=True),
        lax.all_gather(qkv_weight, "fsdp", axis=0, tiled=True),
        lax.all_gather(qkv_bias, "fsdp", axis=0, tiled=True),
        lax.all_gather(rope_freqs, "fsdp", axis=0, tiled=True),
        lax.all_gather(out_weight, "fsdp", axis=0, tiled=True),
        lax.all_gather(out_bias, "fsdp", axis=0, tiled=True),
        lax.all_gather(ln2_gain, "fsdp", axis=0, tiled=True),
        lax.all_gather(ln2_bias, "fsdp", axis=0, tiled=True),
        lax.all_gather(fc1_weight, "fsdp", axis=0, tiled=True),
        lax.all_gather(fc1_bias, "fsdp", axis=0, tiled=True),
        lax.all_gather(fc2_weight, "fsdp", axis=0, tiled=True),
        lax.all_gather(fc2_bias, "fsdp", axis=0, tiled=True),
    )
    (
        gain_one,
        shift_one,
        qkv_mat,
        qkv_shift,
        frequency,
        out_mat,
        out_shift,
        gain_two,
        shift_two,
        fc1_mat,
        fc1_shift,
        fc2_mat,
        fc2_shift,
    ) = gathered
    token_count = layer_in.shape[0]
    inputs = layer_in.astype(jnp.float32)
    row_pos = patch_row.astype(jnp.float32)
    col_pos = patch_col.astype(jnp.float32)
    scale_qk = HD ** (-0.5)
    same_image = image_of[:, None] == image_of[None, :]
    normed_one, norm_one_pull = jax.vjp(
        normed, inputs, gain_one.astype(jnp.float32), shift_one.astype(jnp.float32)
    )
    normed_one_low = normed_one.astype(jnp.bfloat16)
    projected = jnp.dot(
        normed_one_low, qkv_mat, preferred_element_type=jnp.float32
    ) + qkv_shift.astype(jnp.float32)
    queries = projected[:, :D].reshape(token_count, H, HD)
    keys_in = projected[:, D : 2 * D].reshape(token_count, H, HD)
    values_in = projected[:, 2 * D :].reshape(token_count, H, HD)
    rotation = partial(rotate, row_pos=row_pos, col_pos=col_pos)
    (query_rot, key_rot), rope_pull = jax.vjp(
        rotation, queries, keys_in, frequency.astype(jnp.float32)
    )
    query_heads = query_rot.astype(jnp.bfloat16).transpose(1, 0, 2)
    key_heads = key_rot.astype(jnp.bfloat16).transpose(1, 0, 2)
    value_heads = values_in.astype(jnp.bfloat16).transpose(1, 0, 2)

    def head_scores(query_one, key_one):
        scores = (
            jnp.einsum("qd,kd->qk", query_one, key_one, preferred_element_type=jnp.float32)
            * scale_qk
        )
        return jnp.where(same_image, scores, MASKED)

    def head_forward(operands):
        query_one, key_one, value_one = operands
        scores = head_scores(query_one, key_one)
        peak_score = jnp.max(scores, axis=-1, keepdims=True)
        log_total = peak_score + jnp.log(
            jnp.sum(jnp.exp(scores - peak_score), axis=-1, keepdims=True)
        )
        probs = jnp.exp(scores - log_total)
        mixed_one = jnp.dot(
            probs.astype(jnp.bfloat16), value_one, preferred_element_type=jnp.float32
        )
        return (mixed_one, log_total[:, 0])

    mixed_heads, log_totals = lax.map(head_forward, (query_heads, key_heads, value_heads))
    mixed_low = mixed_heads.transpose(1, 0, 2).reshape(token_count, D).astype(jnp.bfloat16)
    middle = (
        inputs
        + jnp.dot(mixed_low, out_mat, preferred_element_type=jnp.float32)
        + out_shift.astype(jnp.float32)
    )
    normed_two, norm_two_pull = jax.vjp(
        normed, middle, gain_two.astype(jnp.float32), shift_two.astype(jnp.float32)
    )
    normed_two_low = normed_two.astype(jnp.bfloat16)
    hidden = jnp.dot(
        normed_two_low, fc1_mat, preferred_element_type=jnp.float32
    ) + fc1_shift.astype(jnp.float32)
    active, gelu_pull = jax.vjp(jax.nn.gelu, hidden)
    active_low = active.astype(jnp.bfloat16)
    result = (
        middle
        + jnp.dot(active_low, fc2_mat, preferred_element_type=jnp.float32)
        + fc2_shift.astype(jnp.float32)
    )
    output = result.astype(jnp.bfloat16)
    again = (
        lax.all_gather(ln1_gain, "fsdp", axis=0, tiled=True),
        lax.all_gather(ln1_bias, "fsdp", axis=0, tiled=True),
        lax.all_gather(qkv_weight, "fsdp", axis=0, tiled=True),
        lax.all_gather(qkv_bias, "fsdp", axis=0, tiled=True),
        lax.all_gather(rope_freqs, "fsdp", axis=0, tiled=True),
        lax.all_gather(out_weight, "fsdp", axis=0, tiled=True),
        lax.all_gather(out_bias, "fsdp", axis=0, tiled=True),
        lax.all_gather(ln2_gain, "fsdp", axis=0, tiled=True),
        lax.all_gather(ln2_bias, "fsdp", axis=0, tiled=True),
        lax.all_gather(fc1_weight, "fsdp", axis=0, tiled=True),
        lax.all_gather(fc1_bias, "fsdp", axis=0, tiled=True),
        lax.all_gather(fc2_weight, "fsdp", axis=0, tiled=True),
        lax.all_gather(fc2_bias, "fsdp", axis=0, tiled=True),
    )
    qkv_back = again[2]
    out_back = again[5]
    fc1_back = again[9]
    fc2_back = again[11]
    upstream = grad_out.astype(jnp.float32)
    grad_fc2 = jnp.einsum("ti,to->io", active_low, grad_out, preferred_element_type=jnp.float32)
    grad_fc2_shift = jnp.sum(upstream, axis=0)
    grad_active = jnp.einsum("to,io->ti", grad_out, fc2_back, preferred_element_type=jnp.float32)
    (grad_hidden,) = gelu_pull(grad_active)
    grad_hidden_low = grad_hidden.astype(jnp.bfloat16)
    grad_fc1 = jnp.einsum(
        "td,th->dh", normed_two_low, grad_hidden_low, preferred_element_type=jnp.float32
    )
    grad_fc1_shift = jnp.sum(grad_hidden_low.astype(jnp.float32), axis=0)
    grad_normed_two = jnp.einsum(
        "th,dh->td", grad_hidden_low, fc1_back, preferred_element_type=jnp.float32
    )
    grad_middle_norm, grad_gain_two, grad_shift_two = norm_two_pull(grad_normed_two)
    grad_middle = upstream + grad_middle_norm
    grad_middle_low = grad_middle.astype(jnp.bfloat16)
    grad_out_shift = jnp.sum(grad_middle_low.astype(jnp.float32), axis=0)
    grad_out_mat = jnp.einsum(
        "ti,to->io", mixed_low, grad_middle_low, preferred_element_type=jnp.float32
    )
    grad_mixed = jnp.einsum(
        "to,io->ti", grad_middle_low, out_back, preferred_element_type=jnp.float32
    )
    grad_mixed_heads = (
        grad_mixed.astype(jnp.bfloat16).reshape(token_count, H, HD).transpose(1, 0, 2)
    )

    def head_backward(operands):
        query_one, key_one, value_one, grad_one, log_total = operands
        scores = head_scores(query_one, key_one)
        probs = jnp.exp(scores - log_total[:, None])
        grad_value = jnp.einsum(
            "qk,qd->kd", probs.astype(jnp.bfloat16), grad_one, preferred_element_type=jnp.float32
        )
        grad_probs = jnp.einsum(
            "qd,kd->qk", grad_one, value_one, preferred_element_type=jnp.float32
        )
        grad_scores = probs * (grad_probs - jnp.sum(probs * grad_probs, axis=-1, keepdims=True))
        grad_scores_low = grad_scores.astype(jnp.bfloat16)
        grad_query = (
            jnp.einsum("qk,kd->qd", grad_scores_low, key_one, preferred_element_type=jnp.float32)
            * scale_qk
        )
        grad_key = (
            jnp.einsum("qk,qd->kd", grad_scores_low, query_one, preferred_element_type=jnp.float32)
            * scale_qk
        )
        return (grad_query, grad_key, grad_value)

    grad_query_heads, grad_key_heads, grad_value_heads = lax.map(
        head_backward, (query_heads, key_heads, value_heads, grad_mixed_heads, log_totals)
    )
    grad_query_rot = grad_query_heads.transpose(1, 0, 2)
    grad_key_rot = grad_key_heads.transpose(1, 0, 2)
    grad_values = grad_value_heads.transpose(1, 0, 2)
    grad_queries, grad_keys, grad_frequency = rope_pull((grad_query_rot, grad_key_rot))
    grad_projected = jnp.concatenate(
        [
            grad_queries.reshape(token_count, D),
            grad_keys.reshape(token_count, D),
            grad_values.reshape(token_count, D),
        ],
        axis=1,
    ).astype(jnp.bfloat16)
    grad_qkv_shift = jnp.sum(grad_projected.astype(jnp.float32), axis=0)
    grad_qkv = jnp.einsum(
        "td,tp->dp", normed_one_low, grad_projected, preferred_element_type=jnp.float32
    )
    grad_normed_one = jnp.einsum(
        "tp,dp->td", grad_projected, qkv_back, preferred_element_type=jnp.float32
    )
    grad_input_norm, grad_gain_one, grad_shift_one = norm_one_pull(grad_normed_one)
    grad_x = (grad_middle + grad_input_norm).astype(jnp.bfloat16)
    owned = (
        lax.psum_scatter(grad_gain_one, "fsdp", scatter_dimension=0, tiled=True),
        lax.psum_scatter(grad_shift_one, "fsdp", scatter_dimension=0, tiled=True),
        lax.psum_scatter(grad_qkv, "fsdp", scatter_dimension=0, tiled=True),
        lax.psum_scatter(grad_qkv_shift, "fsdp", scatter_dimension=0, tiled=True),
        lax.psum_scatter(grad_frequency, "fsdp", scatter_dimension=0, tiled=True),
        lax.psum_scatter(grad_out_mat, "fsdp", scatter_dimension=0, tiled=True),
        lax.psum_scatter(grad_out_shift, "fsdp", scatter_dimension=0, tiled=True),
        lax.psum_scatter(grad_gain_two, "fsdp", scatter_dimension=0, tiled=True),
        lax.psum_scatter(grad_shift_two, "fsdp", scatter_dimension=0, tiled=True),
        lax.psum_scatter(grad_fc1, "fsdp", scatter_dimension=0, tiled=True),
        lax.psum_scatter(grad_fc1_shift, "fsdp", scatter_dimension=0, tiled=True),
        lax.psum_scatter(grad_fc2, "fsdp", scatter_dimension=0, tiled=True),
        lax.psum_scatter(grad_fc2_shift, "fsdp", scatter_dimension=0, tiled=True),
    )
    summed = lax.psum(
        (
            owned[0],
            owned[1],
            owned[2],
            owned[3],
            owned[4],
            owned[5],
            owned[6],
            owned[7],
            owned[8],
            owned[9],
            owned[10],
            owned[11],
            owned[12],
        ),
        "dp",
    )
    return (
        output,
        grad_x,
        summed[0],
        summed[1],
        summed[2],
        summed[3],
        summed[4],
        summed[5],
        summed[6],
        summed[7],
        summed[8],
        summed[9],
        summed[10],
        summed[11],
        summed[12],
    )


def fast_body(
    layer_in,
    ln1_gain,
    ln1_bias,
    qkv_weight,
    qkv_bias,
    rope_freqs,
    out_weight,
    out_bias,
    ln2_gain,
    ln2_bias,
    fc1_weight,
    fc1_bias,
    fc2_weight,
    fc2_bias,
    image_of,
    patch_row,
    patch_col,
    grad_out,
):
    count = lax.axis_size("fsdp")
    seg = D // count
    parts = (ln1_gain, ln1_bias, qkv_bias, rope_freqs, out_bias, ln2_gain, ln2_bias, fc1_bias, fc2_bias)
    small = pack_small(parts, count)
    image, row, col = (a.reshape(-1, 128).astype(jnp.float32) for a in (image_of, patch_row, patch_col))
    output, *kept = forward(
        layer_in, image, row, col, small, (qkv_weight, out_weight, fc1_weight, fc2_weight), count
    )
    grad_x, sums, grad_qkv, grad_out_w, grad_fc1, grad_fc2 = backward(
        layer_in, grad_out, image, row, col, kept, count
    )
    starts, _ = offsets()
    owned = [sums[s : s + m, :seg].reshape(-1) for s, m in zip(starts, SEG_ROWS)]
    owned[FR] = owned[FR].reshape(-1, 2, HD // 2).sum(axis=1).reshape(-1)
    return (
        output,
        grad_x,
        owned[G1],
        owned[B1],
        grad_qkv,
        owned[QB],
        owned[FR],
        grad_out_w,
        owned[OB],
        owned[G2],
        owned[B2],
        grad_fc1,
        owned[F1B],
        grad_fc2,
        owned[F2B],
    )


def fits(mesh, tokens):
    count, planes = mesh.shape["fsdp"], mesh.shape["dp"]
    return count == 8 and planes == 4 and tokens == 640 * count * planes


def solution(mesh):
    in_specs = (
        P(("fsdp", "dp"), None),
        P("fsdp"),
        P("fsdp"),
        P("fsdp", None),
        P("fsdp"),
        P("fsdp"),
        P("fsdp", None),
        P("fsdp"),
        P("fsdp"),
        P("fsdp"),
        P("fsdp", None),
        P("fsdp"),
        P("fsdp", None),
        P("fsdp"),
        P(("fsdp", "dp")),
        P(("fsdp", "dp")),
        P(("fsdp", "dp")),
        P(("fsdp", "dp"), None),
    )
    out_specs = (
        P(("fsdp", "dp"), None),
        P(("fsdp", "dp"), None),
        P("fsdp"),
        P("fsdp"),
        P("fsdp", None),
        P("fsdp"),
        P("fsdp"),
        P("fsdp", None),
        P("fsdp"),
        P("fsdp"),
        P("fsdp"),
        P("fsdp", None),
        P("fsdp"),
        P("fsdp", None),
        P("fsdp"),
    )
    def step(*arguments):
        chosen = fast_body if fits(mesh, arguments[0].shape[0]) else body
        mapped = jax.shard_map(chosen, mesh=mesh, in_specs=in_specs, out_specs=out_specs, check_vma=False)
        return mapped(*arguments)

    return step
```
